32 devices in a mesh: grid: 8 (over y, x, core), sub: 4 (over z).
Axes of the slice: x: 2, y: 2, z: 4, core: 2. Of those that a mesh axis runs over, the one named last changes fastest.
Arguments:
- grid_x: bfloat16 [65536, 512], P(('grid', 'sub')), may hold values from -6 to 6
- mesh_h: bfloat16 [2048, 512], P(('grid', 'sub')), may hold values from -6 to 6
- gain_grid: float32 [512], replicated, may hold values from 0.1 to 1.9
- gain_mesh: float32 [512], replicated, may hold values from 0.1 to 1.9
- w_query: bfloat16 [512, 512], replicated, may hold values from -0.25 to 0.25
- w_key: bfloat16 [512, 512], replicated, may hold values from -0.25 to 0.25
- w_value: bfloat16 [512, 512], replicated, may hold values from -0.25 to 0.25
- w_out: bfloat16 [512, 512], replicated, may hold values from -0.25 to 0.25
- edge_bias: float32 [2048, 384], P(('grid', 'sub')), may hold values from -9 to 300
- neighbours: int32 [2048, 96], P(('grid', 'sub')), may hold values from 0 to 767, as said below
- valid: int32 [2048, 96], P(('grid', 'sub')), may hold values from 0 to 1, as said below
- send_rows: int32 [32, 3, 4, 64], P(('grid', 'sub')), may hold values from 0 to 2047, as said below
- out_grad: bfloat16 [2048, 512], P(('grid', 'sub')), may hold values from -24 to 24
Outputs:
- mesh_out: bfloat16 [2048, 512], P(('grid', 'sub'))
- mesh_grad: bfloat16 [2048, 512], P(('grid', 'sub'))
- grid_grad: bfloat16 [65536, 512], P(('grid', 'sub'))
- weight_grads: float32 [4, 512, 512], replicated
The draws below stay inside these ranges and needn't reach their ends.
Inputs may be any that keep to these rules, and one draw needn't show every extreme that they name: `send_rows`: for each source device, slab offset and destination sub index the 64 local rows are distinct; rows sent to the slab below (o = 0) lie in the lower half of the device's 2048 rows, rows sent to the slab above (o = 2) in the upper half. `neighbours`: a slot (o * 4 + s) * 64 + t names row t of what device s of slab g - o + 1 sends to the node's device; slots of slabs outside the grid are never named; the 96 entries of a node are distinct; some slots are named by no node. The first two edges of every node are valid.
All inputs are finite; a program needn't handle non-finite values.
Results may differ from the reference program's by a relative error of at most 0.009.
Values may be sent and summed in bfloat16 or wider, within the bound.
A program may use at most 128 MiB of HBM per device.

```python
import jax
import jax.numpy as jnp
from jax import lax

FEATURE_WIDTH = 512
HEADS = 4
GRID_NEIGHBOURS = 96
G_DEV = 2048
MESH_PER_SHARD = 64
RANKS = 32
CAP = 64
SLOTS = 768
HEAD_DIM = 128
GRID = 65536
MESH = 2048
N_GRID = 8
N_SUB = 4


def pair_counts(key):
    count_key = jax.random.fold_in(key, 11)
    lowest = max(2, CAP // 2)
    counts = jax.random.randint(count_key, (RANKS, 3, N_SUB), lowest, CAP + 1)
    rank_ids = jnp.arange(RANKS)[:, None, None]
    offsets = jnp.arange(3)[None, :, None]
    subs = jnp.arange(N_SUB)[None, None, :]
    slab = rank_ids // N_SUB
    own_sub = rank_ids % N_SUB
    counts = jnp.where((offsets == 1) & (subs == own_sub), CAP, counts)
    source_slab = slab - offsets + 1
    inside = (source_slab >= 0) & (source_slab < N_GRID)
    return jnp.where(inside, counts, 0)


def draw_send_rows(key, part):
    subkeys = jax.random.split(jax.random.fold_in(key, 23), RANKS * 3 * N_SUB)
    half_rows = jax.vmap(lambda subkey: jax.random.permutation(subkey, G_DEV // 2)[:CAP])(subkeys)
    full_rows = jax.vmap(lambda subkey: jax.random.permutation(jax.random.fold_in(subkey, 5), G_DEV)[:CAP])(subkeys)
    half_rows = half_rows.reshape(RANKS, 3, N_SUB, CAP)
    full_rows = full_rows.reshape(RANKS, 3, N_SUB, CAP)
    offsets = jnp.arange(3)[None, :, None, None]
    picked = jnp.where(offsets == 0, half_rows, jnp.where(offsets == 2, half_rows + G_DEV // 2, full_rows))
    return picked.astype(jnp.int32)


def draw_neighbours(key, part):
    counts = pair_counts(key)
    slot_iota = jnp.arange(SLOTS)
    offset_of = slot_iota // (N_SUB * CAP)
    sub_of = slot_iota // CAP % N_SUB
    within = slot_iota % CAP
    owner = jnp.arange(MESH) // MESH_PER_SHARD
    limit = counts[owner[:, None], offset_of[None, :], sub_of[None, :]]
    used = within[None, :] < limit
    top_value = (1 << 30) // SLOTS
    noise = jax.random.randint(jax.random.fold_in(key, 37), (MESH, SLOTS), 0, top_value)
    ranked = jnp.where(used, noise * SLOTS + slot_iota[None, :], -1)
    chosen = lax.top_k(ranked, GRID_NEIGHBOURS)[1]
    return chosen.astype(jnp.int32)


def draw_valid(key, part):
    levels = jax.random.randint(jax.random.fold_in(key, 41), (MESH, GRID_NEIGHBOURS), 0, 5)
    column = jnp.arange(GRID_NEIGHBOURS)[None, :]
    return jnp.where((levels > 0) | (column < 2), 1, 0).astype(jnp.int32)


def draw_edge_bias(key, part):
    normal_key = jax.random.fold_in(jax.random.fold_in(key, 53), 0)
    base = jax.random.normal(normal_key, (MESH, HEADS, GRID_NEIGHBOURS), jnp.float32)
    base = jnp.clip(base, -4.0, 4.0)
    return base.reshape(MESH, HEADS * GRID_NEIGHBOURS).astype(jnp.float32)


def steps_of(rng, dims, cuts, least, high):
    loudness = 1.0
    for axis_at, shards_of in cuts:
        draws = jax.random.uniform(jax.random.fold_in(jax.random.fold_in(rng, 6), axis_at), (shards_of,), jnp.float32, least / len(cuts), high / len(cuts))
        loudness = loudness * jnp.repeat(jnp.exp(draws), dims[axis_at] // shards_of).reshape((-1,) + (1,) * (len(dims) - 1 - axis_at))
    return loudness


def scatter_about(stream_key, extent, deviation, bound, cuts=(), kind=jnp.bfloat16):
    values = deviation * jax.random.normal(stream_key, extent, jnp.float32)
    if cuts:
        values = values * steps_of(stream_key, extent, cuts, -0.22, 0.18)
    return jnp.clip(values, -bound, bound).astype(kind)


def setup_inputs(seed: int = 0) -> dict:
    streams_of = jax.random.split(jax.random.key(seed), 14)
    return {
        "grid_x": scatter_about(streams_of[0], (GRID, FEATURE_WIDTH), 1.0, 6.0, ((0, 32),)),
        "mesh_h": scatter_about(streams_of[1], (MESH, FEATURE_WIDTH), 1.0, 6.0, ((0, 32),)),
        "gain_grid": jnp.clip(1.0 + 0.18 * jax.random.normal(streams_of[2], (FEATURE_WIDTH,), jnp.float32), 0.1, 1.9),
        "gain_mesh": jnp.clip(1.0 + 0.18 * jax.random.normal(streams_of[3], (FEATURE_WIDTH,), jnp.float32), 0.1, 1.9),
        "w_query": scatter_about(streams_of[4], (FEATURE_WIDTH, FEATURE_WIDTH), FEATURE_WIDTH ** -0.5, 0.25),
        "w_key": scatter_about(streams_of[5], (FEATURE_WIDTH, FEATURE_WIDTH), FEATURE_WIDTH ** -0.5, 0.25),
        "w_value": scatter_about(streams_of[6], (FEATURE_WIDTH, FEATURE_WIDTH), FEATURE_WIDTH ** -0.5, 0.25),
        "w_out": scatter_about(streams_of[7], (FEATURE_WIDTH, FEATURE_WIDTH), FEATURE_WIDTH ** -0.5, 0.25),
        "edge_bias": draw_edge_bias(jax.random.fold_in(streams_of[13], 71), 0),
        "neighbours": draw_neighbours(jax.random.fold_in(streams_of[13], 71), 0),
        "valid": draw_valid(jax.random.fold_in(streams_of[13], 71), 0),
        "send_rows": draw_send_rows(jax.random.fold_in(streams_of[13], 71), 0),
        "out_grad": scatter_about(streams_of[12], (MESH, FEATURE_WIDTH), 4.0, 24.0, ((0, 32),)),
    }


EPSILON = 1e-06
NEG_FILL = -1e+30

def normalize(values_in, gain_row):
    widened = values_in.astype(jnp.float32)
    factor = lax.rsqrt(lax.optimization_barrier(jnp.mean(widened * widened, axis=-1, keepdims=True)) + EPSILON)
    return (widened, factor, (widened * factor * gain_row).astype(jnp.bfloat16))

def normalize_back(widened, factor, gain_row, upstream):
    scaled = gain_row * upstream
    inner_mean = lax.optimization_barrier(jnp.mean(widened * scaled, axis=-1, keepdims=True))
    return factor * scaled - widened * factor ** 3 * inner_mean

def reference(grid_x, mesh_h, gain_grid, gain_mesh, w_query, w_key, w_value, w_out, edge_bias, neighbours, valid, send_rows, out_grad):
    logit_scale = HEAD_DIM ** (-0.5)
    grid_wide, grid_factor, grid_normed = normalize(grid_x, gain_grid)
    keys = jnp.dot(grid_normed, w_key, preferred_element_type=jnp.float32).astype(jnp.bfloat16)
    values = jnp.dot(grid_normed, w_value, preferred_element_type=jnp.float32).astype(jnp.bfloat16)
    mesh_wide, mesh_factor, mesh_normed = normalize(mesh_h, gain_mesh)
    queries = (jnp.dot(mesh_normed, w_query, preferred_element_type=jnp.float32) * logit_scale).astype(jnp.bfloat16)
    offsets = jnp.arange(3, dtype=jnp.int32)[:, None]
    subs = jnp.arange(N_SUB, dtype=jnp.int32)[None, :]

    def per_device(state_pair, rank_id):
        grid_acc, grad_acc = state_pair
        slab = (rank_id // N_SUB).astype(jnp.int32)
        own_sub = (rank_id % N_SUB).astype(jnp.int32)
        src_slab = jnp.clip(slab - offsets + 1, 0, N_GRID - 1).astype(jnp.int32)
        src_rank = (src_slab * N_SUB + subs).astype(jnp.int32)
        rows = send_rows[src_rank, jnp.broadcast_to(offsets, (3, N_SUB)), own_sub]
        point_ids = (src_rank[:, :, None] * G_DEV + rows).reshape(SLOTS).astype(jnp.int32)
        row_start = (rank_id * MESH_PER_SHARD).astype(jnp.int32)
        node_q = lax.dynamic_slice_in_dim(queries, row_start, MESH_PER_SHARD, 0)
        node_wide = lax.dynamic_slice_in_dim(mesh_wide, row_start, MESH_PER_SHARD, 0)
        node_factor = lax.dynamic_slice_in_dim(mesh_factor, row_start, MESH_PER_SHARD, 0)
        node_normed = lax.dynamic_slice_in_dim(mesh_normed, row_start, MESH_PER_SHARD, 0)
        node_grad = lax.dynamic_slice_in_dim(out_grad, row_start, MESH_PER_SHARD, 0)
        mesh_node_bias = lax.dynamic_slice_in_dim(edge_bias, row_start, MESH_PER_SHARD, 0).reshape(MESH_PER_SHARD, HEADS, GRID_NEIGHBOURS)
        node_nbr = lax.dynamic_slice_in_dim(neighbours, row_start, MESH_PER_SHARD, 0)
        node_valid = lax.dynamic_slice_in_dim(valid, row_start, MESH_PER_SHARD, 0)
        edge_points = point_ids[node_nbr]
        edge_key_rows = keys[edge_points].astype(jnp.float32).reshape(MESH_PER_SHARD, GRID_NEIGHBOURS, HEADS, HEAD_DIM)
        edge_value_rows = values[edge_points].astype(jnp.float32).reshape(MESH_PER_SHARD, GRID_NEIGHBOURS, HEADS, HEAD_DIM)
        query_head_rows = node_q.astype(jnp.float32).reshape(MESH_PER_SHARD, HEADS, HEAD_DIM)
        score_matrix = jnp.einsum('fog,flog->fol', query_head_rows, edge_key_rows) + mesh_node_bias
        live_mask = (node_valid == 1)[:, None, :]
        row_peak = lax.optimization_barrier(jnp.max(jnp.where(live_mask, score_matrix, NEG_FILL), axis=2, keepdims=True))
        exp_terms = jnp.exp(jnp.where(live_mask, score_matrix - row_peak, NEG_FILL))
        attn_probs = exp_terms / lax.optimization_barrier(jnp.sum(exp_terms, axis=2, keepdims=True))
        probabilities_batch = attn_probs.astype(jnp.bfloat16)
        attended_rows = jnp.einsum('bao,boai->bai', probabilities_batch.astype(jnp.float32), edge_value_rows).reshape(MESH_PER_SHARD, FEATURE_WIDTH).astype(jnp.bfloat16)
        out_rows = (node_wide + jnp.dot(attended_rows, w_out, preferred_element_type=jnp.float32)).astype(jnp.bfloat16)
        grad_wo = jnp.dot(attended_rows.T, node_grad, preferred_element_type=jnp.float32)
        att_grad = jnp.dot(node_grad, w_out.T, preferred_element_type=jnp.float32).astype(jnp.bfloat16)
        head_gradient = att_grad.astype(jnp.float32).reshape(MESH_PER_SHARD, HEADS, HEAD_DIM)
        probability_gradient = jnp.einsum('fog,flog->fol', head_gradient, edge_value_rows)
        score_gradient = (attn_probs * (probability_gradient - lax.optimization_barrier(jnp.sum(attn_probs * probability_gradient, axis=2, keepdims=True)))).astype(jnp.bfloat16)
        query_gradient = (jnp.einsum('bao,boai->bai', score_gradient.astype(jnp.float32), edge_key_rows) * logit_scale).reshape(MESH_PER_SHARD, FEATURE_WIDTH).astype(jnp.bfloat16)
        key_per_edge = jnp.einsum('iuw,iuy->iwuy', score_gradient.astype(jnp.float32), query_head_rows).reshape(MESH_PER_SHARD * GRID_NEIGHBOURS, FEATURE_WIDTH)
        value_per_edge = jnp.einsum('iuw,iuy->iwuy', probabilities_batch.astype(jnp.float32), head_gradient).reshape(MESH_PER_SHARD * GRID_NEIGHBOURS, FEATURE_WIDTH)
        slot_ids = node_nbr.reshape(MESH_PER_SHARD * GRID_NEIGHBOURS)
        key_part = jax.ops.segment_sum(key_per_edge, slot_ids, num_segments=SLOTS).astype(jnp.bfloat16)
        value_part = jax.ops.segment_sum(value_per_edge, slot_ids, num_segments=SLOTS).astype(jnp.bfloat16)
        sent_normed = grid_normed[point_ids]
        grad_wk = jnp.dot(sent_normed.T, key_part, preferred_element_type=jnp.float32)
        grad_wv = jnp.dot(sent_normed.T, value_part, preferred_element_type=jnp.float32)
        slot_back = jnp.dot(key_part, w_key.T, preferred_element_type=jnp.float32) + jnp.dot(value_part, w_value.T, preferred_element_type=jnp.float32)
        grid_acc = grid_acc.at[point_ids].add(slot_back)
        grad_wq = jnp.dot(node_normed.T, query_gradient, preferred_element_type=jnp.float32)
        normed_grad = jnp.dot(query_gradient, w_query.T, preferred_element_type=jnp.float32)
        grad_rows = (node_grad.astype(jnp.float32) + normalize_back(node_wide, node_factor, gain_mesh, normed_grad)).astype(jnp.bfloat16)
        grad_acc = grad_acc + jnp.stack([grad_wq, grad_wk, grad_wv, grad_wo])
        return ((grid_acc, grad_acc), (out_rows, grad_rows))
    initial = (jnp.zeros((GRID, FEATURE_WIDTH), jnp.float32), jnp.zeros((4, FEATURE_WIDTH, FEATURE_WIDTH), jnp.float32))
    (grid_acc, grad_acc), (out_rows, grad_rows) = lax.scan(per_device, initial, jnp.arange(RANKS, dtype=jnp.int32))
    grid_grad = normalize_back(grid_wide, grid_factor, gain_grid, grid_acc).astype(jnp.bfloat16)
    return (out_rows.reshape(MESH, FEATURE_WIDTH), grad_rows.reshape(MESH, FEATURE_WIDTH), grid_grad, grad_acc)
```

```python
import functools

import jax
import jax.numpy as jnp
from jax import lax
from jax.experimental import pallas as pl
from jax.experimental.pallas import tpu as pltpu
from jax.sharding import PartitionSpec as P

EPSILON = 1e-06
NEG_FILL = -1e30
F32 = jnp.float32
BF16 = jnp.bfloat16
NN = (((1,), (0,)), ((), ()))
NT = (((1,), (1,)), ((), ()))
TN = (((0,), (0,)), ((), ()))
LANES = 128
ROWS = 24


def dot(a, b, dims=NN):
    return lax.dot_general(a, b, dims, preferred_element_type=F32)


def normalize(values_in, gain_row):
    widened = values_in.astype(F32)
    factor = lax.rsqrt(jnp.mean(widened * widened, axis=-1, keepdims=True) + EPSILON)
    return (widened, factor, (widened * factor * gain_row).astype(BF16))


def normalize_back(widened, factor, gain_row, upstream):
    scaled = gain_row * upstream
    inner_mean = jnp.mean(widened * scaled, axis=-1, keepdims=True)
    return factor * scaled - widened * factor**3 * inner_mean


def layer(
    n_grid,
    n_sub,
    grid_x, mesh_h, gain_g, gain_m, w_q, w_k, w_v, w_o, bias, nbr, valid, rows, out_grad,
    returned_out, gathered, mesh_out, mesh_grad,
    x_s, mesh_s, gg_s, gm_s, wq_s, wk_s, wv_s, wo_s, bias_s, nbr_s, valid_s, rows_s, og_s,
    packet, arrived, slot_back, returned,
    edge_rows, dense, slot_of, q_s, ag_s, mn_s, k_s, v_s, att_s, qg_s, back_k, back_v, mo_s, mg_s,
    part, core_out, core_in, chip_acc, chip_out, chip_in, sub_acc, sub_out, sub_in, whole,
    load_sem, fwd_send, fwd_recv, back_send, back_recv,
    core_send, core_recv, chip_send, chip_recv, sub_send, sub_recv,
    subg_send, subg_recv, chipg_send, chipg_recv, coreg_send, coreg_recv, store_sem,
):
    g = lax.axis_index("grid")
    c = lax.axis_index("sub")
    core = lax.rem(g, 2)
    chip = lax.div(g, 2)
    chips = n_grid // 2
    other_core = g + 1 - 2 * core
    points, width = x_s.shape
    nodes = mesh_s.shape[0]
    slots_per = rows_s.shape[3]
    fanout = nbr_s.shape[1]
    heads = bias_s.shape[1] // fanout
    head = width // heads
    slots = 3 * n_sub * slots_per
    scale = head ** (-0.5)
    half = points // 2

    loads = {}
    pairs = (
        ("rows", rows, rows_s), ("x", grid_x, x_s), ("gg", gain_g, gg_s), ("nbr", nbr, nbr_s),
        ("bias", bias, bias_s), ("valid", valid, valid_s), ("mesh", mesh_h, mesh_s),
        ("gm", gain_m, gm_s), ("wq", w_q, wq_s), ("og", out_grad, og_s), ("wo", w_o, wo_s),
        ("wk", w_k, wk_s), ("wv", w_v, wv_s),
    )
    for at, (name, source, target) in enumerate(pairs):
        loads[name] = pltpu.make_async_copy(source, target, load_sem.at[at])
        loads[name].start()

    def wrap(value, size):
        return lax.rem(value + size, size)

    def remote(source, target, send, recv, to_grid, to_sub):
        return pltpu.make_async_remote_copy(
            src_ref=source, dst_ref=target, send_sem=send, recv_sem=recv,
            device_id={"grid": to_grid, "sub": to_sub}, device_id_type=pl.DeviceIdType.MESH,
        )

    barrier = pltpu.get_barrier_semaphore()
    peers = [
        (wrap(g + o, n_grid), wrap(c + k, n_sub))
        for k in range(n_sub) for o in (-1, 0, 1) if (o, k) != (0, 0)
    ] + [(lax.rem(chip + j, chips) * 2 + core, c) for j in range(1, chips)]
    for to_grid, to_sub in peers:
        pl.semaphore_signal(
            barrier, inc=1, device_id={"grid": to_grid, "sub": to_sub},
            device_id_type=pl.DeviceIdType.MESH,
        )

    far_first = sorted(range(n_sub), key=lambda k: -min(k, n_sub - k))

    loads["rows"].wait()
    eye = (
        lax.broadcasted_iota(jnp.int32, (slots_per, slots_per), 0)
        == lax.broadcasted_iota(jnp.int32, (slots_per, slots_per), 1)
    )
    pl.semaphore_wait(barrier, len(peers))
    forward = {}
    for o in (0, 2, 1):
        low, span = (0, half) if o == 0 else (half, points - half) if o == 2 else (0, points)
        lane = lax.broadcasted_iota(jnp.int32, (slots_per, span), 1) + low
        picks = []
        for s in range(n_sub):
            row = rows_s[0, o, pl.ds(s, 1), :].astype(F32)
            column = jnp.sum(jnp.where(eye, row, 0.0), axis=1, keepdims=True).astype(jnp.int32)
            picks.append(jnp.where(lane == column, 1.0, 0.0).astype(BF16))
        onehot = jnp.concatenate(picks, axis=0)
        if o == 0:
            loads["x"].wait()
            loads["gg"].wait()
        chosen = dot(onehot, x_s[pl.ds(low, span), :])
        factor = lax.rsqrt(jnp.mean(chosen * chosen, axis=-1, keepdims=True) + EPSILON)
        packet[o] = (chosen * factor * gg_s[...]).astype(BF16).reshape(n_sub, slots_per, width)
        for k in far_first:
            if (o, k) == (1, 0):
                continue
            to_sub = lax.rem(c + k, n_sub)
            forward[o, k] = remote(
                packet.at[o, to_sub], arrived.at[k, o],
                fwd_send.at[o * n_sub + k], fwd_recv.at[o * n_sub + k],
                wrap(g + o - 1, n_grid), to_sub,
            )
            forward[o, k].start()
    arrived[0, 1] = packet[1, c]

    for name in ("nbr", "bias", "valid"):
        loads[name].wait()
    named = nbr_s[...]
    offset_of = lax.div(named, n_sub * slots_per)
    sub_of = lax.rem(lax.div(named, slots_per), n_sub)
    turn = lax.rem(c - sub_of + n_sub, n_sub)
    slot_of[...] = (turn * 3 + offset_of) * slots_per + lax.rem(named, slots_per)
    edge_rows[...] = jnp.zeros(edge_rows.shape, F32)
    for h in range(heads):
        values = bias_s[:, h * fanout:(h + 1) * fanout]
        high = values.astype(BF16).astype(F32)
        middle = (values - high).astype(BF16).astype(F32)
        edge_rows[pl.ds(h, nodes, stride=ROWS), :fanout] = high
        edge_rows[pl.ds(8 + h, nodes, stride=ROWS), :fanout] = middle
        edge_rows[pl.ds(16 + h, nodes, stride=ROWS), :fanout] = values - high - middle
    edge_rows[pl.ds(heads, nodes, stride=ROWS), :fanout] = jnp.where(valid_s[...] == 1, 1.0, 0.0)

    slot_ids = lax.broadcasted_iota(jnp.int32, (slots, fanout), 0)
    group = 8

    def spread(step, carry):
        for inner in range(group):
            node = step * group + inner
            names = slot_ids == slot_of[pl.ds(node, 1), :]
            onehot = jnp.where(names, 1.0, 0.0).astype(BF16)
            at = pl.multiple_of(node * ROWS, 8)
            spread_rows = dot(edge_rows[pl.ds(at, ROWS), :fanout].astype(BF16), onehot, NT)
            total = (spread_rows[16:24] + spread_rows[8:16]) + spread_rows[:8]
            for tile in range(slots // LANES):
                dense[tile, pl.ds(pl.multiple_of(node * 8, 8), 8), :] = (
                    total[:, tile * LANES:(tile + 1) * LANES]
                )
        return carry

    lax.fori_loop(0, nodes // group, spread, 0)

    for name in ("mesh", "gm", "wq", "og", "wo", "wk", "wv"):
        loads[name].wait()
    mesh_wide, mesh_factor, mesh_normed = normalize(mesh_s[...], gm_s[...])
    mn_s[...] = mesh_normed
    q_s[...] = (dot(mesh_normed, wq_s[...]) * scale).astype(BF16)
    ag_s[...] = dot(og_s[...], wo_s[...], NT).astype(BF16)

    for move in forward.values():
        move.wait_recv()
    rows_in = arrived[...].reshape(slots, width)
    k_s[...] = dot(rows_in, wk_s[...]).astype(BF16)
    v_s[...] = dot(rows_in, wv_s[...]).astype(BF16)

    def spread_of(row):
        return jnp.concatenate(
            [dense[tile, pl.ds(row, nodes, stride=8), :] for tile in range(slots // LANES)], axis=1
        )

    live = spread_of(heads) > 0.5
    for h in range(heads):
        mine = slice(h * head, (h + 1) * head)
        queries, keys, values, att_grad = q_s[:, mine], k_s[:, mine], v_s[:, mine], ag_s[:, mine]
        scores = dot(queries, keys, NT) + spread_of(h)
        peak = jnp.max(jnp.where(live, scores, NEG_FILL), axis=1, keepdims=True)
        terms = jnp.exp(jnp.where(live, scores - peak, NEG_FILL))
        probs = terms / jnp.sum(terms, axis=1, keepdims=True)
        probs_b = probs.astype(BF16)
        att_s[:, mine] = dot(probs_b, values).astype(BF16)
        prob_grads = dot(att_grad, values, NT)
        score_grads = (
            probs * (prob_grads - jnp.sum(probs * prob_grads, axis=1, keepdims=True))
        ).astype(BF16)
        qg_s[:, mine] = (dot(score_grads, keys) * scale).astype(BF16)
        back_k[:, mine] = dot(score_grads, queries, TN).astype(BF16)
        back_v[:, mine] = dot(probs_b, att_grad, TN).astype(BF16)

    backward = {}
    turn_rows = 3 * slots_per
    for k in far_first:
        here = slice(k * turn_rows, (k + 1) * turn_rows)
        total = dot(back_k[here, :], wk_s[...], NT) + dot(back_v[here, :], wv_s[...], NT)
        slot_back[k] = total.astype(BF16).reshape(3, slots_per, width)
        for o in range(3):
            if (o, k) == (1, 0):
                continue
            backward[o, k] = remote(
                slot_back.at[k, o], returned.at[o, c],
                back_send.at[o * n_sub + k], back_recv.at[o * n_sub + k],
                wrap(g + 1 - o, n_grid), wrap(c - k, n_sub),
            )
            backward[o, k].start()
    returned[1, pl.ds(c, 1)] = slot_back[0, 1][None]

    half_rows = width // 2
    chunks = part.shape[0]
    block = half_rows // chips
    moves = {}

    def core_stage(ch, first, second):
        for m, grad in enumerate((first, second)):
            part[ch, m] = grad.reshape(2, half_rows, width)
            core_out[ch, m] = part[ch, m, 1 - core].astype(BF16)
        move = remote(
            core_out.at[ch], core_in.at[ch], core_send.at[ch], core_recv.at[ch], other_core, c
        )
        move.start()
        moves["core", ch] = [move]

    def chip_stage(ch):
        moves["core", ch][0].wait_recv()
        for j in range(chips):
            for m in range(2):
                at = pl.ds(j * block, block)
                total = part[ch, m, core, at, :] + core_in[ch, m, at, :].astype(F32)
                chip_acc[ch, j, m] = total
                chip_out[ch, j, m] = total.astype(BF16)
        moves["chip", ch] = []
        for j in range(1, chips):
            to_chip = lax.rem(chip + j, chips)
            move = remote(
                chip_out.at[ch, to_chip], chip_in.at[ch, j],
                chip_send.at[ch, j], chip_recv.at[ch, j], to_chip * 2 + core, c,
            )
            move.start()
            moves["chip", ch].append(move)

    def sub_stage(ch):
        for move in moves["chip", ch]:
            move.wait_recv()
        for m in range(2):
            total = chip_acc[ch, chip, m]
            for j in range(1, chips):
                total = total + chip_in[ch, j, m].astype(F32)
            for z in range(n_sub):
                piece = total[:, z * (width // n_sub):(z + 1) * (width // n_sub)]
                sub_acc[ch, z, m] = piece
                sub_out[ch, z, m] = piece.astype(BF16)
        moves["sub", ch] = []
        for k in far_first[:-1]:
            to_sub = lax.rem(c + k, n_sub)
            move = remote(
                sub_out.at[ch, to_sub], sub_in.at[ch, k],
                sub_send.at[ch, k], sub_recv.at[ch, k], g, to_sub,
            )
            move.start()
            moves["sub", ch].append(move)

    def sub_gather(ch):
        for move in moves["sub", ch]:
            move.wait_recv()
        total = sub_acc[ch, c]
        for k in range(1, n_sub):
            total = total + sub_in[ch, k].astype(F32)
        whole[ch, chip, pl.ds(c, 1)] = total.astype(BF16)[None]
        moves["subg", ch] = []
        for k in far_first[:-1]:
            move = remote(
                whole.at[ch, chip, c], whole.at[ch, chip, c],
                subg_send.at[ch, k], subg_recv.at[ch, k], g, lax.rem(c + k, n_sub),
            )
            move.start()
            moves["subg", ch].append(move)

    def chip_gather(ch):
        for move in moves["subg", ch]:
            move.wait_recv()
        moves["chipg", ch] = []
        for j in range(1, chips):
            move = remote(
                whole.at[ch, chip], whole.at[ch, chip],
                chipg_send.at[ch, j], chipg_recv.at[ch, j],
                lax.rem(chip + j, chips) * 2 + core, c,
            )
            move.start()
            moves["chipg", ch].append(move)

    def core_gather(ch):
        for move in moves["chipg", ch]:
            move.wait_recv()
        move = remote(
            whole.at[ch], gathered.at[ch, core], coreg_send.at[ch], coreg_recv.at[ch],
            other_core, c,
        )
        move.start()
        moves["coreg", ch] = [move]
        own = pltpu.make_async_copy(whole.at[ch], gathered.at[ch, core], store_sem.at[ch])
        own.start()
        stores.append(own)

    stores = []
    core_stage(0, dot(mn_s[...], qg_s[...], TN), dot(att_s[...], og_s[...], TN))
    core_stage(1, dot(rows_in, back_k[...], TN), dot(rows_in, back_v[...], TN))
    for ch in range(chunks):
        chip_stage(ch)

    mo_s[...] = (mesh_wide + dot(att_s[...], wo_s[...])).astype(BF16)
    mesh_normed_grad = dot(qg_s[...], wq_s[...], NT)
    mg_s[...] = (
        og_s[...].astype(F32)
        + normalize_back(mesh_wide, mesh_factor, gm_s[...], mesh_normed_grad)
    ).astype(BF16)
    for at, (source, target) in enumerate(((mo_s, mesh_out), (mg_s, mesh_grad))):
        own = pltpu.make_async_copy(source, target, store_sem.at[chunks + at])
        own.start()
        stores.append(own)

    for ch in range(chunks):
        sub_stage(ch)
    for ch in range(chunks):
        sub_gather(ch)
    for ch in range(chunks):
        chip_gather(ch)
    for move in backward.values():
        move.wait_recv()
    own = pltpu.make_async_copy(returned, returned_out, store_sem.at[chunks + 2])
    own.start()
    stores.append(own)
    for ch in range(chunks):
        core_gather(ch)
    for ch in range(chunks):
        moves["coreg", ch][0].wait_recv()
    for own in stores:
        own.wait()
    for move in [*forward.values(), *backward.values()] + sum(moves.values(), []):
        move.wait_send()


def finish(
    returned, gathered, mesh_out_in, mesh_grad_in, grid_x, gain_g, rows,
    mesh_out, mesh_grad, grid_grad, weight_grads,
    returned_s, gathered_s, mo_s, mg_s, x_s, gg_s, rows_s, flat, gx_s, w_s, load_sem, store_sem,
):
    points, width = x_s.shape
    n_sub, slots_per = rows_s.shape[2:]
    block = n_sub * slots_per
    chunks, _, chips, _, mats, part_rows, part_lanes = gathered_s.shape
    pieces = x_s.shape[0] // 4
    loads = {}
    pairs = [
        ("rows", rows, rows_s), ("gg", gain_g, gg_s), ("back", returned, returned_s),
    ] + [
        (("x", b), grid_x.at[pl.ds(b * pieces, pieces)], x_s.at[pl.ds(b * pieces, pieces)])
        for b in range(4)
    ] + [
        (("w", ch), gathered.at[ch], gathered_s.at[ch]) for ch in range(chunks)
    ] + [("mo", mesh_out_in, mo_s), ("mg", mesh_grad_in, mg_s)]
    for at, (name, source, target) in enumerate(pairs):
        loads[name] = pltpu.make_async_copy(source, target, load_sem.at[at])
        loads[name].start()
    stores = []

    def store(source, target):
        move = pltpu.make_async_copy(source, target, store_sem.at[len(stores)])
        move.start()
        stores.append(move)

    loads["rows"].wait()
    for o in range(3):
        for s in range(n_sub):
            at = o * block + s * slots_per
            flat[:, at:at + slots_per] = rows_s[0, o, pl.ds(s, 1), :]
    loads["gg"].wait()
    loads["back"].wait()
    back = returned_s[...].reshape(3 * block, width)
    for b in range(4):
        loads["x", b].wait()
        at = slice(b * pieces, (b + 1) * pieces)
        low = 0 if b < 2 else block
        point = lax.broadcasted_iota(jnp.int32, (pieces, 2 * block), 0) + b * pieces
        onehot = jnp.where(point == flat[:, low:low + 2 * block], 1.0, 0.0).astype(BF16)
        normed_grad = dot(onehot, back[low:low + 2 * block])
        wide = x_s[at, :].astype(F32)
        factor = lax.rsqrt(jnp.mean(wide * wide, axis=-1, keepdims=True) + EPSILON)
        gx_s[at, :] = normalize_back(wide, factor, gg_s[...], normed_grad).astype(BF16)
        store(gx_s.at[pl.ds(b * pieces, pieces)], grid_grad.at[pl.ds(b * pieces, pieces)])
    loads["mo"].wait()
    store(mo_s, mesh_out)
    loads["mg"].wait()
    store(mg_s, mesh_grad)
    half_rows = width // 2
    for ch, order in enumerate(((0, 3), (1, 2))):
        loads["w", ch].wait()
        for m, matrix in enumerate(order):
            for core in range(2):
                for j in range(chips):
                    at = core * half_rows + j * part_rows
                    for z in range(n_sub):
                        w_s[matrix, at:at + part_rows, z * part_lanes:(z + 1) * part_lanes] = (
                            gathered_s[ch, core, j, z, m].astype(F32)
                        )
            store(w_s.at[matrix], weight_grads.at[matrix])
    for move in stores:
        move.wait()


def shards(
    n_grid, n_sub,
    grid_x, mesh_h, gain_grid, gain_mesh, w_query, w_key, w_value, w_out,
    edge_bias, neighbours, valid, send_rows, out_grad,
):
    points, width = grid_x.shape
    nodes = mesh_h.shape[0]
    slots_per = send_rows.shape[3]
    fanout = neighbours.shape[1]
    slots = 3 * n_sub * slots_per
    chips = n_grid // 2
    chunks, mats = 2, 2
    half_rows = width // 2
    block, lanes = half_rows // chips, width // n_sub
    anywhere = pl.BlockSpec(memory_space=pl.ANY)
    dma = pltpu.SemaphoreType.DMA
    gain_grid, gain_mesh = gain_grid.reshape(1, width), gain_mesh.reshape(1, width)
    operands = (
        grid_x, mesh_h, gain_grid, gain_mesh, w_query, w_key, w_value, w_out,
        edge_bias, neighbours, valid, send_rows, out_grad,
    )
    blocks = (3, n_sub, slots_per, width)
    turns = (n_sub, 3, slots_per, width)
    node_rows = pltpu.VMEM((nodes, width), BF16)
    slot_rows = pltpu.VMEM((slots, width), BF16)
    piece = (chunks, n_sub, mats, block, lanes)
    returned, gathered, mesh_out, mesh_grad = pl.pallas_call(
        functools.partial(layer, n_grid, n_sub),
        in_specs=[anywhere] * len(operands),
        out_specs=[anywhere] * 4,
        out_shape=[
            jax.ShapeDtypeStruct(blocks, BF16),
            jax.ShapeDtypeStruct((chunks, 2, chips, n_sub, mats, block, lanes), BF16),
            jax.ShapeDtypeStruct((nodes, width), BF16),
            jax.ShapeDtypeStruct((nodes, width), BF16),
        ],
        scratch_shapes=[pltpu.VMEM(a.shape, a.dtype) for a in operands] + [
            pltpu.VMEM(blocks, BF16), pltpu.VMEM(turns, BF16),
            pltpu.VMEM(turns, BF16), pltpu.VMEM(blocks, BF16),
            pltpu.VMEM((nodes * ROWS, LANES), F32),
            pltpu.VMEM((slots // LANES, nodes * 8, LANES), F32),
            pltpu.VMEM((nodes, fanout), jnp.int32),
            node_rows, node_rows, node_rows, slot_rows, slot_rows, node_rows, node_rows,
            slot_rows, slot_rows, node_rows, node_rows,
            pltpu.VMEM((chunks, mats, 2, half_rows, width), F32),
            pltpu.VMEM((chunks, mats, half_rows, width), BF16),
            pltpu.VMEM((chunks, mats, half_rows, width), BF16),
            pltpu.VMEM((chunks, chips, mats, block, width), F32),
            pltpu.VMEM((chunks, chips, mats, block, width), BF16),
            pltpu.VMEM((chunks, chips, mats, block, width), BF16),
            pltpu.VMEM(piece, F32), pltpu.VMEM(piece, BF16), pltpu.VMEM(piece, BF16),
            pltpu.VMEM((chunks, chips, n_sub, mats, block, lanes), BF16),
            dma((len(operands),)),
            dma((3 * n_sub,)), dma((3 * n_sub,)), dma((3 * n_sub,)), dma((3 * n_sub,)),
            dma((chunks,)), dma((chunks,)),
            dma((chunks, chips)), dma((chunks, chips)),
            dma((chunks, n_sub)), dma((chunks, n_sub)),
            dma((chunks, n_sub)), dma((chunks, n_sub)),
            dma((chunks, chips)), dma((chunks, chips)),
            dma((chunks,)), dma((chunks,)),
            dma((chunks + 3,)),
        ],
        compiler_params=pltpu.CompilerParams(collective_id=0, has_side_effects=True),
        name="layer",
    )(*operands)
    return pl.pallas_call(
        finish,
        in_specs=[anywhere] * 7,
        out_specs=[anywhere] * 4,
        out_shape=[
            jax.ShapeDtypeStruct((nodes, width), BF16),
            jax.ShapeDtypeStruct((nodes, width), BF16),
            jax.ShapeDtypeStruct((points, width), BF16),
            jax.ShapeDtypeStruct((chunks * mats, width, width), F32),
        ],
        scratch_shapes=[
            pltpu.VMEM(blocks, BF16),
            pltpu.VMEM((chunks, 2, chips, n_sub, mats, block, lanes), BF16),
            node_rows, node_rows,
            pltpu.VMEM((points, width), BF16), pltpu.VMEM((1, width), F32),
            pltpu.VMEM(send_rows.shape, jnp.int32), pltpu.VMEM((1, slots), jnp.int32),
            pltpu.VMEM((points, width), BF16),
            pltpu.VMEM((chunks * mats, width, width), F32),
            dma((9 + chunks,)), dma((6 + chunks * mats,)),
        ],
        name="finish",
    )(returned, gathered, mesh_out, mesh_grad, grid_x, gain_grid, send_rows)


def solution(mesh):
    by_device = P(("grid", "sub"), None)
    in_specs = (
        by_device, by_device, P(), P(), P(), P(), P(), P(), by_device, by_device, by_device,
        P(("grid", "sub"), None, None, None), by_device,
    )
    out_specs = (by_device, by_device, by_device, P())
    body = functools.partial(shards, mesh.shape["grid"], mesh.shape["sub"])
    return jax.shard_map(body, mesh=mesh, in_specs=in_specs, out_specs=out_specs, check_vma=False)
```

```python
import functools

import jax
import jax.numpy as jnp
from jax import lax
from jax.experimental import pallas as pl
from jax.experimental.pallas import tpu as pltpu
from jax.sharding import PartitionSpec as P

EPSILON = 1e-06
NEG_FILL = -1e30
F32 = jnp.float32
BF16 = jnp.bfloat16
NN = (((1,), (0,)), ((), ()))
NT = (((1,), (1,)), ((), ()))
TN = (((0,), (0,)), ((), ()))
LANES = 128
ROWS = 24


def dot(a, b, dims=NN):
    return lax.dot_general(a, b, dims, preferred_element_type=F32)


def normalize(values_in, gain_row):
    widened = values_in.astype(F32)
    factor = lax.rsqrt(jnp.mean(widened * widened, axis=-1, keepdims=True) + EPSILON)
    return (widened, factor, (widened * factor * gain_row).astype(BF16))


def normalize_back(widened, factor, gain_row, upstream):
    scaled = gain_row * upstream
    inner_mean = jnp.mean(widened * scaled, axis=-1, keepdims=True)
    return factor * scaled - widened * factor**3 * inner_mean


def layer(
    n_grid,
    n_sub,
    grid_x, mesh_h, gain_g, gain_m, w_q, w_k, w_v, w_o, bias, nbr, valid, rows, out_grad,
    returned_out, gathered, mesh_out, mesh_grad,
    x_s, mesh_s, gg_s, gm_s, wq_s, wk_s, wv_s, wo_s, bias_s, nbr_s, valid_s, rows_s, og_s,
    packet, arrived, slot_back, returned,
    edge_rows, dense, slot_of, q_s, ag_s, k_s, v_s, att_s, qg_s, back_k, back_v, mo_s, mg_s,
    known, factor_send, factor_in, factor_part, factor_out_s, factor_core,
    part, core_out, core_in, chip_acc, chip_out, chip_in, sub_acc, sub_out, sub_in, whole,
    load_sem, fwd_send, fwd_recv, back_send, back_recv,
    known_send, known_recv, factor_ssem, factor_rsem, core_send, core_recv, chip_send, chip_recv, sub_send, sub_recv,
    subg_send, subg_recv, chipg_send, chipg_recv, coreg_send, coreg_recv, store_sem,
):
    g = lax.axis_index("grid")
    c = lax.axis_index("sub")
    core = lax.rem(g, 2)
    chip = lax.div(g, 2)
    chips = n_grid // 2
    other_core = g + 1 - 2 * core
    points, width = x_s.shape
    nodes = mesh_s.shape[0]
    slots_per = rows_s.shape[3]
    fanout = nbr_s.shape[1]
    heads = bias_s.shape[1] // fanout
    head = width // heads
    slots = 3 * n_sub * slots_per
    scale = head ** (-0.5)
    half = points // 2

    loads = {}
    pairs = (
        ("rows", rows, rows_s), ("x", grid_x, x_s), ("gg", gain_g, gg_s), ("nbr", nbr, nbr_s),
        ("bias", bias, bias_s), ("valid", valid, valid_s), ("mesh", mesh_h, mesh_s),
        ("gm", gain_m, gm_s), ("wq", w_q, wq_s), ("og", out_grad, og_s), ("wo", w_o, wo_s),
        ("wk", w_k, wk_s), ("wv", w_v, wv_s),
    )
    for at, (name, source, target) in enumerate(pairs):
        loads[name] = pltpu.make_async_copy(source, target, load_sem.at[at])
        loads[name].start()

    def wrap(value, size):
        return lax.rem(value + size, size)

    def remote(source, target, send, recv, to_grid, to_sub):
        return pltpu.make_async_remote_copy(
            src_ref=source, dst_ref=target, send_sem=send, recv_sem=recv,
            device_id={"grid": to_grid, "sub": to_sub}, device_id_type=pl.DeviceIdType.MESH,
        )

    barrier = pltpu.get_barrier_semaphore()
    peers = [
        (wrap(g + o, n_grid), wrap(c + k, n_sub))
        for k in range(n_sub) for o in (-1, 0, 1) if (o, k) != (0, 0)
    ] + [(lax.rem(chip + j, chips) * 2 + core, c) for j in range(1, chips)]
    for to_grid, to_sub in peers:
        pl.semaphore_signal(
            barrier, inc=1, device_id={"grid": to_grid, "sub": to_sub},
            device_id_type=pl.DeviceIdType.MESH,
        )

    far_first = sorted(range(n_sub), key=lambda k: -min(k, n_sub - k))

    loads["rows"].wait()
    eye = (
        lax.broadcasted_iota(jnp.int32, (slots_per, slots_per), 0)
        == lax.broadcasted_iota(jnp.int32, (slots_per, slots_per), 1)
    )
    forward = {}
    for o in (0, 2, 1):
        low, span = (0, half) if o == 0 else (half, points - half) if o == 2 else (0, points)
        lane = lax.broadcasted_iota(jnp.int32, (slots_per, span), 1) + low
        picks = []
        for s in range(n_sub):
            row = rows_s[0, o, pl.ds(s, 1), :].astype(F32)
            column = jnp.sum(jnp.where(eye, row, 0.0), axis=1, keepdims=True).astype(jnp.int32)
            picks.append(jnp.where(lane == column, 1.0, 0.0).astype(BF16))
        onehot = jnp.concatenate(picks, axis=0)
        if o == 0:
            loads["x"].wait()
            loads["gg"].wait()
        chosen = dot(onehot, x_s[pl.ds(low, span), :])
        factor = lax.rsqrt(jnp.mean(chosen * chosen, axis=-1, keepdims=True) + EPSILON)
        packet[o] = (chosen * factor * gg_s[...]).astype(BF16).reshape(n_sub, slots_per, width)
        if o == 0:
            pl.semaphore_wait(barrier, len(peers))
        for k in far_first:
            if (o, k) == (1, 0):
                continue
            to_sub = lax.rem(c + k, n_sub)
            forward[o, k] = remote(
                packet.at[o, to_sub], arrived.at[k, o],
                fwd_send.at[o * n_sub + k], fwd_recv.at[o * n_sub + k],
                wrap(g + o - 1, n_grid), to_sub,
            )
            forward[o, k].start()
    arrived[0, 1] = packet[1, c]

    for name in ("mesh", "gm", "og"):
        loads[name].wait()
    mesh_wide, mesh_factor, mesh_normed = normalize(mesh_s[...], gm_s[...])
    known[0, pl.ds(chip, 1)] = og_s[...][None]
    known[1, pl.ds(chip, 1)] = mesh_normed[None]
    known_moves = {}
    for ch in range(2):
        known_moves["known", ch] = []
        for j in range(1, chips):
            to_chip = lax.rem(chip + j, chips)
            move = remote(
                known.at[ch, chip], known.at[ch, chip], known_send.at[ch, j], known_recv.at[ch, j],
                to_chip * 2 + core, c,
            )
            move.start()
            known_moves["known", ch].append(move)

    for name in ("nbr", "bias", "valid"):
        loads[name].wait()
    named = nbr_s[...]
    offset_of = lax.div(named, n_sub * slots_per)
    sub_of = lax.rem(lax.div(named, slots_per), n_sub)
    turn = lax.rem(c - sub_of + n_sub, n_sub)
    slot_of[...] = (turn * 3 + offset_of) * slots_per + lax.rem(named, slots_per)
    edge_rows[...] = jnp.zeros(edge_rows.shape, F32)
    for h in range(heads):
        values = bias_s[:, h * fanout:(h + 1) * fanout]
        high = values.astype(BF16).astype(F32)
        middle = (values - high).astype(BF16).astype(F32)
        edge_rows[pl.ds(h, nodes, stride=ROWS), :fanout] = high
        edge_rows[pl.ds(8 + h, nodes, stride=ROWS), :fanout] = middle
        edge_rows[pl.ds(16 + h, nodes, stride=ROWS), :fanout] = values - high - middle
    edge_rows[pl.ds(heads, nodes, stride=ROWS), :fanout] = jnp.where(valid_s[...] == 1, 1.0, 0.0)

    slot_ids = lax.broadcasted_iota(jnp.int32, (slots, fanout), 0)
    group = 8

    def spread(step, carry):
        for inner in range(group):
            node = step * group + inner
            names = slot_ids == slot_of[pl.ds(node, 1), :]
            onehot = jnp.where(names, 1.0, 0.0).astype(BF16)
            at = pl.multiple_of(node * ROWS, 8)
            spread_rows = dot(edge_rows[pl.ds(at, ROWS), :fanout].astype(BF16), onehot, NT)
            total = (spread_rows[16:24] + spread_rows[8:16]) + spread_rows[:8]
            for tile in range(slots // LANES):
                dense[tile, pl.ds(pl.multiple_of(node * 8, 8), 8), :] = (
                    total[:, tile * LANES:(tile + 1) * LANES]
                )
        return carry

    lax.fori_loop(0, nodes // group, spread, 0)

    for name in ("wq", "wo", "wk", "wv"):
        loads[name].wait()
    q_s[...] = (dot(mesh_normed, wq_s[...]) * scale).astype(BF16)
    ag_s[...] = dot(og_s[...], wo_s[...], NT).astype(BF16)

    for move in forward.values():
        move.wait_recv()
    rows_in = arrived[...].reshape(slots, width)
    k_s[...] = dot(rows_in, wk_s[...]).astype(BF16)
    v_s[...] = dot(rows_in, wv_s[...]).astype(BF16)

    def spread_of(row):
        return jnp.concatenate(
            [dense[tile, pl.ds(row, nodes, stride=8), :] for tile in range(slots // LANES)], axis=1
        )

    live = spread_of(heads) > 0.5
    for h in range(heads):
        mine = slice(h * head, (h + 1) * head)
        queries, keys, values, att_grad = q_s[:, mine], k_s[:, mine], v_s[:, mine], ag_s[:, mine]
        scores = dot(queries, keys, NT) + spread_of(h)
        peak = jnp.max(jnp.where(live, scores, NEG_FILL), axis=1, keepdims=True)
        terms = jnp.exp(jnp.where(live, scores - peak, NEG_FILL))
        probs = terms / jnp.sum(terms, axis=1, keepdims=True)
        probs_b = probs.astype(BF16)
        att_s[:, mine] = dot(probs_b, values).astype(BF16)
        prob_grads = dot(att_grad, values, NT)
        score_grads = (
            probs * (prob_grads - jnp.sum(probs * prob_grads, axis=1, keepdims=True))
        ).astype(BF16)
        qg_s[:, mine] = (dot(score_grads, keys) * scale).astype(BF16)
        back_k[:, mine] = dot(score_grads, queries, TN).astype(BF16)
        back_v[:, mine] = dot(probs_b, att_grad, TN).astype(BF16)

    backward = {}
    turn_rows = 3 * slots_per

    def turn_back(k):
        here = slice(k * turn_rows, (k + 1) * turn_rows)
        total = dot(back_k[here, :], wk_s[...], NT) + dot(back_v[here, :], wv_s[...], NT)
        slot_back[k] = total.astype(BF16).reshape(3, slots_per, width)

    def send_home(k, o):
        backward[o, k] = remote(
            slot_back.at[k, o], returned.at[o, c],
            back_send.at[o * n_sub + k], back_recv.at[o * n_sub + k],
            wrap(g + 1 - o, n_grid), wrap(c - k, n_sub),
        )
        backward[o, k].start()

    half_rows = width // 2
    chunks = whole.shape[0]
    block = half_rows // chips
    lanes = width // n_sub
    chip_bits, sub_bits = chips.bit_length() - 1, n_sub.bit_length() - 1
    moves = {}
    stores = []

    def flip(index, bit):
        return index + bit - 2 * bit * lax.rem(lax.div(index, bit), 2)

    def reverse(index, bits):
        total = 0
        for t in range(bits):
            total = total + lax.rem(lax.div(index, 2**t), 2) * 2 ** (bits - 1 - t)
        return total

    chip_of = (chip, reverse(chip, chip_bits))
    part_of = lax.rem(c, 2)

    def start(key, *move):
        moves.setdefault(key, []).append(remote(*move))
        moves[key][-1].start()

    def arrive(key):
        for move in moves[key]:
            move.wait_recv()

    def factor_out(ch):
        source = (att_s, qg_s)[ch]
        piece = width // chips
        for j in range(chips):
            factor_send[ch, j] = source[:, j * piece:(j + 1) * piece]
        for j in range(1, chips):
            to_chip = lax.rem(chip + j, chips)
            start(
                ("factor", ch), factor_send.at[ch, to_chip], factor_in.at[ch, chip],
                factor_ssem.at[ch, j], factor_rsem.at[ch, j], to_chip * 2 + core, c,
            )
        factor_in[ch, pl.ds(chip, 1)] = factor_send[ch, pl.ds(chip, 1)]

    def factor_sum(ch):
        arrive(("factor", ch))
        arrive(("known", ch))
        total = dot(
            factor_in[ch].reshape(chips * nodes, width // chips),
            known[ch].reshape(chips * nodes, width), TN,
        )
        factor_part[ch] = total.reshape(2, block, width)
        factor_out_s[ch] = factor_part[ch, 1 - core].astype(BF16)
        start(
            ("core", ch), factor_out_s.at[ch], factor_core.at[ch],
            core_send.at[ch], core_recv.at[ch], other_core, c,
        )

    def core_stage(ch, grad):
        m = ch - 2
        part[m] = grad.reshape(2, half_rows, width)
        core_out[m] = part[m, 1 - core].astype(BF16)
        start(
            ("core", ch), core_out.at[m], core_in.at[m],
            core_send.at[ch], core_recv.at[ch], other_core, c,
        )

    def chip_stage(ch):
        m = ch - 2
        arrive(("core", ch))
        for j in range(chips):
            at = pl.ds(j * block, block)
            total = part[m, core, at, :] + core_in[m, at, :].astype(F32)
            chip_acc[m, j] = total
            chip_out[m, j] = total.astype(BF16)
        for j in range(1, chips):
            to_chip = lax.rem(chip + j, chips)
            start(
                ("chip", ch), chip_out.at[m, to_chip], chip_in.at[m, j],
                chip_send.at[m, j], chip_recv.at[m, j], to_chip * 2 + core, c,
            )

    def sub_step(ch, t):
        keep = n_sub >> (t + 1)
        low = 0
        for earlier in range(t):
            low = low + lax.rem(lax.div(c, 2**earlier), 2) * (n_sub >> (earlier + 1))
        bit = lax.rem(lax.div(c, 2**t), 2)
        for i in range(keep):
            sub_out[ch, t, i] = sub_acc[ch, low + (1 - bit) * keep + i].astype(BF16)
        start(
            ("sub", ch, t), sub_out.at[ch, t, pl.ds(0, keep)], sub_in.at[ch, t, pl.ds(0, keep)],
            sub_send.at[ch, t], sub_recv.at[ch, t], g, flip(c, 2**t),
        )

    def sub_sum(ch, t):
        keep = n_sub >> (t + 1)
        arrive(("sub", ch, t))
        low = 0
        for earlier in range(t + 1):
            low = low + lax.rem(lax.div(c, 2**earlier), 2) * (n_sub >> (earlier + 1))
        for i in range(keep):
            sub_acc[ch, low + i] = sub_acc[ch, low + i] + sub_in[ch, t, i].astype(F32)

    def sub_first(ch):
        if ch < 2:
            arrive(("core", ch))
            total = factor_part[ch, core] + factor_core[ch].astype(F32)
        else:
            arrive(("chip", ch))
            total = chip_acc[ch - 2, chip]
            for j in range(1, chips):
                total = total + chip_in[ch - 2, j].astype(F32)
        for z in range(n_sub):
            sub_acc[ch, z] = total[:, z * lanes:(z + 1) * lanes]
        sub_step(ch, 0)

    def sub_next(ch):
        for t in range(1, sub_bits):
            sub_sum(ch, t - 1)
            sub_step(ch, t)

    def gather_step(ch, t):
        held = n_sub >> (t + 1)
        at_chip = chip_of[0] * (1 - part_of) + chip_of[1] * part_of
        low = 0
        for earlier in range(1, t + 1):
            low = low + lax.rem(lax.div(c, 2**earlier), 2) * (n_sub >> (earlier + 1))
        piece = whole.at[ch, part_of, at_chip, pl.ds(low, held)]
        start(
            ("subg", ch, t), piece, piece, subg_send.at[ch, t], subg_recv.at[ch, t],
            g, flip(c, 2**t),
        )

    def sub_gather(ch):
        t = sub_bits - 1
        sub_sum(ch, t)
        spot = reverse(c, sub_bits)
        at_chip = chip_of[0] * (1 - part_of) + chip_of[1] * part_of
        whole[ch, part_of, at_chip, pl.ds(lax.rem(spot, n_sub // 2), 1)] = (
            sub_acc[ch, spot].astype(BF16)[None]
        )
        gather_step(ch, t)

    def sub_gather_next(ch):
        for t in range(sub_bits - 2, -1, -1):
            arrive(("subg", ch, t + 1))
            gather_step(ch, t)

    def chip_step(ch, t):
        for p in range(2):
            bit = 2**t if p == 0 else 2 ** (chip_bits - 1 - t)
            low = lax.div(chip_of[p], 2**t) * 2**t
            piece = whole.at[ch, p, pl.ds(low, 2**t)]
            start(
                ("chipg", ch, t), piece, piece, chipg_send.at[ch, p, t], chipg_recv.at[ch, p, t],
                flip(chip, bit) * 2 + core, c,
            )

    def chip_gather(ch):
        arrive(("subg", ch, 0))
        chip_step(ch, 0)

    def chip_gather_next(ch):
        for t in range(1, chip_bits):
            arrive(("chipg", ch, t - 1))
            chip_step(ch, t)

    def core_gather(ch):
        arrive(("chipg", ch, chip_bits - 1))
        start(
            ("coreg", ch), whole.at[ch], gathered.at[ch, core],
            coreg_send.at[ch], coreg_recv.at[ch], other_core, c,
        )
        own = pltpu.make_async_copy(whole.at[ch], gathered.at[ch, core], store_sem.at[ch])
        own.start()
        stores.append(own)

    moves.update(known_moves)
    far, near = far_first[0], far_first[1:-1]
    home = [(k, o) for k in (far, *near) for o in range(3)] + [(0, 0), (0, 2)]

    def send_next():
        if home:
            send_home(*home.pop(0))

    factor_out(0)
    factor_out(1)
    turn_back(far)
    send_next()
    core_stage(2, dot(rows_in, back_k[...], TN))
    core_stage(3, dot(rows_in, back_v[...], TN))
    factor_sum(0)
    factor_sum(1)
    chip_stage(2)
    chip_stage(3)
    sub_first(0)
    sub_first(1)
    send_next()
    for k in (*near, 0):
        turn_back(k)
    returned[1, pl.ds(c, 1)] = slot_back[0, 1][None]
    sub_next(0)
    sub_next(1)
    send_next()
    mo_s[...] = (mesh_wide + dot(att_s[...], wo_s[...])).astype(BF16)
    mesh_normed_grad = dot(qg_s[...], wq_s[...], NT)
    mg_s[...] = (
        og_s[...].astype(F32)
        + normalize_back(mesh_wide, mesh_factor, gm_s[...], mesh_normed_grad)
    ).astype(BF16)
    for at, (source, target) in enumerate(((mo_s, mesh_out), (mg_s, mesh_grad))):
        own = pltpu.make_async_copy(source, target, store_sem.at[chunks + at])
        own.start()
        stores.append(own)

    stages = (
        (sub_first, 2), (sub_gather, 0), (sub_gather, 1), None,
        (sub_first, 3), (sub_next, 2), (sub_gather_next, 0), (sub_gather_next, 1), None,
        (sub_next, 3), (sub_gather, 2), (chip_gather, 0), (chip_gather, 1), None,
        (sub_gather, 3), (sub_gather_next, 2), (chip_gather_next, 0), (chip_gather_next, 1), None,
        (sub_gather_next, 3), (chip_gather, 2), None,
        (chip_gather, 3), None, (chip_gather_next, 2), None,
        (core_gather, 0), (core_gather, 1), None,
        (chip_gather_next, 3), None, (core_gather, 2), (core_gather, 3),
    )
    for stage in stages:
        if stage is None:
            send_next()
        else:
            stage[0](stage[1])
    while home:
        send_next()
    for move in backward.values():
        move.wait_recv()
    own = pltpu.make_async_copy(returned, returned_out, store_sem.at[chunks + 2])
    own.start()
    stores.append(own)
    for ch in range(chunks):
        arrive(("coreg", ch))
    for own in stores:
        own.wait()
    for move in [*forward.values(), *backward.values()] + sum(moves.values(), []):
        move.wait_send()


def finish(
    returned, gathered, mesh_out_in, mesh_grad_in, grid_x, gain_g, rows,
    mesh_out, mesh_grad, grid_grad, weight_grads,
    returned_s, gathered_s, mo_s, mg_s, x_s, gg_s, rows_s, flat, gx_s, w_s, load_sem, store_sem,
):
    points, width = x_s.shape
    n_sub, slots_per = rows_s.shape[2:]
    block = n_sub * slots_per
    chunks, _, _, chips, _, part_rows, part_lanes = gathered_s.shape
    pieces = points // 4
    loads = {}
    pairs = [
        ("rows", rows, rows_s), ("gg", gain_g, gg_s), ("back", returned, returned_s),
    ] + [
        (("x", b), grid_x.at[pl.ds(b * pieces, pieces)], x_s.at[pl.ds(b * pieces, pieces)])
        for b in range(4)
    ] + [
        (("w", ch), gathered.at[ch], gathered_s.at[ch]) for ch in range(chunks)
    ] + [("mo", mesh_out_in, mo_s), ("mg", mesh_grad_in, mg_s)]
    for at, (name, source, target) in enumerate(pairs):
        loads[name] = pltpu.make_async_copy(source, target, load_sem.at[at])
        loads[name].start()
    stores = []

    def store(source, target):
        move = pltpu.make_async_copy(source, target, store_sem.at[len(stores)])
        move.start()
        stores.append(move)

    loads["rows"].wait()
    for o in range(3):
        for s in range(n_sub):
            at = o * block + s * slots_per
            flat[:, at:at + slots_per] = rows_s[0, o, pl.ds(s, 1), :]
    loads["gg"].wait()
    loads["back"].wait()
    back = returned_s[...].reshape(3 * block, width)
    for b in range(4):
        loads["x", b].wait()
        at = slice(b * pieces, (b + 1) * pieces)
        low = 0 if b < 2 else block
        point = lax.broadcasted_iota(jnp.int32, (pieces, 2 * block), 0) + b * pieces
        onehot = jnp.where(point == flat[:, low:low + 2 * block], 1.0, 0.0).astype(BF16)
        normed_grad = dot(onehot, back[low:low + 2 * block])
        wide = x_s[at, :].astype(F32)
        factor = lax.rsqrt(jnp.mean(wide * wide, axis=-1, keepdims=True) + EPSILON)
        gx_s[at, :] = normalize_back(wide, factor, gg_s[...], normed_grad).astype(BF16)
        store(gx_s.at[pl.ds(b * pieces, pieces)], grid_grad.at[pl.ds(b * pieces, pieces)])
    loads["mo"].wait()
    store(mo_s, mesh_out)
    loads["mg"].wait()
    store(mg_s, mesh_grad)
    half_rows = width // 2
    chip_bits = chips.bit_length() - 1

    def flipped(index, bits):
        return sum((index >> t & 1) << (bits - 1 - t) for t in range(bits))

    def piece_of(ch, core, j, z):
        part, at = divmod(z, n_sub // 2)
        return gathered_s[ch, core, part, flipped(j, chip_bits) if part else j, at].astype(F32)

    for ch, matrix in enumerate((3, 0, 1, 2)):
        loads["w", ch].wait()
        for j in range(chips):
            for z in range(n_sub):
                columns = slice(z * part_lanes, (z + 1) * part_lanes)
                cores = [piece_of(ch, core, j, z) for core in range(2)]
                if ch < 2:
                    both = jnp.concatenate(cores, axis=0)
                    span = slice(2 * j * part_rows, 2 * (j + 1) * part_rows)
                    if ch == 0:
                        w_s[matrix, span, columns] = both
                    else:
                        w_s[matrix, columns, span] = both.T
                else:
                    for core in range(2):
                        at = core * half_rows + j * part_rows
                        w_s[matrix, at:at + part_rows, columns] = cores[core]
        store(w_s.at[matrix], weight_grads.at[matrix])
    for move in stores:
        move.wait()


def shards(
    n_grid, n_sub,
    grid_x, mesh_h, gain_grid, gain_mesh, w_query, w_key, w_value, w_out,
    edge_bias, neighbours, valid, send_rows, out_grad,
):
    points, width = grid_x.shape
    nodes = mesh_h.shape[0]
    slots_per = send_rows.shape[3]
    fanout = neighbours.shape[1]
    slots = 3 * n_sub * slots_per
    chips = n_grid // 2
    chunks = 4
    half_rows = width // 2
    block, lanes = half_rows // chips, width // n_sub
    anywhere = pl.BlockSpec(memory_space=pl.ANY)
    dma = pltpu.SemaphoreType.DMA
    gain_grid, gain_mesh = gain_grid.reshape(1, width), gain_mesh.reshape(1, width)
    operands = (
        grid_x, mesh_h, gain_grid, gain_mesh, w_query, w_key, w_value, w_out,
        edge_bias, neighbours, valid, send_rows, out_grad,
    )
    blocks = (3, n_sub, slots_per, width)
    turns = (n_sub, 3, slots_per, width)
    node_rows = pltpu.VMEM((nodes, width), BF16)
    slot_rows = pltpu.VMEM((slots, width), BF16)
    chip_bits, sub_bits = chips.bit_length() - 1, n_sub.bit_length() - 1
    pieces = (chunks, 2, 2, chips, n_sub // 2, block, lanes)
    returned, gathered, mesh_out, mesh_grad = pl.pallas_call(
        functools.partial(layer, n_grid, n_sub),
        in_specs=[anywhere] * len(operands),
        out_specs=[anywhere] * 4,
        out_shape=[
            jax.ShapeDtypeStruct(blocks, BF16),
            jax.ShapeDtypeStruct(pieces, BF16),
            jax.ShapeDtypeStruct((nodes, width), BF16),
            jax.ShapeDtypeStruct((nodes, width), BF16),
        ],
        scratch_shapes=[pltpu.VMEM(a.shape, a.dtype) for a in operands] + [
            pltpu.VMEM(blocks, BF16), pltpu.VMEM(turns, BF16),
            pltpu.VMEM(turns, BF16), pltpu.VMEM(blocks, BF16),
            pltpu.VMEM((nodes * ROWS, LANES), F32),
            pltpu.VMEM((slots // LANES, nodes * 8, LANES), F32),
            pltpu.VMEM((nodes, fanout), jnp.int32),
            node_rows, node_rows, slot_rows, slot_rows, node_rows, node_rows,
            slot_rows, slot_rows, node_rows, node_rows,
            pltpu.VMEM((2, chips, nodes, width), BF16),
            pltpu.VMEM((2, chips, nodes, width // chips), BF16),
            pltpu.VMEM((2, chips, nodes, width // chips), BF16),
            pltpu.VMEM((2, 2, block, width), F32),
            pltpu.VMEM((2, block, width), BF16), pltpu.VMEM((2, block, width), BF16),
            pltpu.VMEM((2, 2, half_rows, width), F32),
            pltpu.VMEM((2, half_rows, width), BF16), pltpu.VMEM((2, half_rows, width), BF16),
            pltpu.VMEM((2, chips, block, width), F32),
            pltpu.VMEM((2, chips, block, width), BF16), pltpu.VMEM((2, chips, block, width), BF16),
            pltpu.VMEM((chunks, n_sub, block, lanes), F32),
            pltpu.VMEM((chunks, sub_bits, n_sub // 2, block, lanes), BF16),
            pltpu.VMEM((chunks, sub_bits, n_sub // 2, block, lanes), BF16),
            pltpu.VMEM(pieces[:1] + pieces[2:], BF16),
            dma((len(operands),)),
            dma((3 * n_sub,)), dma((3 * n_sub,)), dma((3 * n_sub,)), dma((3 * n_sub,)),
            dma((2, chips)), dma((2, chips)), dma((2, chips)), dma((2, chips)),
            dma((chunks,)), dma((chunks,)), dma((2, chips)), dma((2, chips)),
            dma((chunks, sub_bits)), dma((chunks, sub_bits)),
            dma((chunks, sub_bits)), dma((chunks, sub_bits)),
            dma((chunks, 2, chip_bits)), dma((chunks, 2, chip_bits)),
            dma((chunks,)), dma((chunks,)),
            dma((chunks + 3,)),
        ],
        compiler_params=pltpu.CompilerParams(collective_id=0, has_side_effects=True),
        name="layer",
    )(*operands)
    return pl.pallas_call(
        finish,
        in_specs=[anywhere] * 7,
        out_specs=[anywhere] * 4,
        out_shape=[
            jax.ShapeDtypeStruct((nodes, width), BF16),
            jax.ShapeDtypeStruct((nodes, width), BF16),
            jax.ShapeDtypeStruct((points, width), BF16),
            jax.ShapeDtypeStruct((chunks, width, width), F32),
        ],
        scratch_shapes=[
            pltpu.VMEM(blocks, BF16),
            pltpu.VMEM(pieces, BF16),
            node_rows, node_rows,
            pltpu.VMEM((points, width), BF16), pltpu.VMEM((1, width), F32),
            pltpu.VMEM(send_rows.shape, jnp.int32), pltpu.VMEM((1, slots), jnp.int32),
            pltpu.VMEM((points, width), BF16),
            pltpu.VMEM((chunks, width, width), F32),
            dma((9 + chunks,)), dma((6 + chunks,)),
        ],
        name="finish",
    )(returned, gathered, mesh_out, mesh_grad, grid_x, gain_grid, send_rows)


def solution(mesh):
    by_device = P(("grid", "sub"), None)
    in_specs = (
        by_device, by_device, P(), P(), P(), P(), P(), P(), by_device, by_device, by_device,
        P(("grid", "sub"), None, None, None), by_device,
    )
    out_specs = (by_device, by_device, by_device, P())
    body = functools.partial(shards, mesh.shape["grid"], mesh.shape["sub"])
    return jax.shard_map(body, mesh=mesh, in_specs=in_specs, out_specs=out_specs, check_vma=False)
```

```python
import functools

import jax
import jax.numpy as jnp
from jax import lax
from jax.experimental import pallas as pl
from jax.experimental.pallas import tpu as pltpu
from jax.sharding import PartitionSpec as P

EPSILON = 1e-06
NEG_FILL = -1e30
F32 = jnp.float32
BF16 = jnp.bfloat16
NN = (((1,), (0,)), ((), ()))
NT = (((1,), (1,)), ((), ()))
TN = (((0,), (0,)), ((), ()))
LANES = 128
LIMIT = 32 * 2**20
VMEM_BYTES = 67043328
ROWS = 24


def dot(a, b, dims=NN):
    return lax.dot_general(a, b, dims, preferred_element_type=F32)


def normalize(values_in, gain_row):
    widened = values_in.astype(F32)
    factor = lax.rsqrt(jnp.mean(widened * widened, axis=-1, keepdims=True) + EPSILON)
    return (widened, factor, (widened * factor * gain_row).astype(BF16))


def normalize_back(widened, factor, gain_row, upstream):
    scaled = gain_row * upstream
    inner_mean = jnp.mean(widened * scaled, axis=-1, keepdims=True)
    return factor * scaled - widened * factor**3 * inner_mean


def layer(
    n_grid,
    n_sub,
    grid_x, mesh_h, gain_g, gain_m, w_q, w_k, w_v, w_o, bias, nbr, valid, rows, out_grad,
    grid_grad, gathered, mgathered, mo_s, mg_s,
    x_s, mesh_s, gg_s, gm_s, wq_s, wk_s, wv_s, wo_s, bias_s, nbr_s, valid_s, rows_s, og_s,
    packet, arrived, rows_t, slot_back, returned, flat, onehot_t, factor_s,
    edge_rows, dense, slot_of, q_s, ag_s, k_s, v_s, att_s, qg_s, back_k, back_v,
    known, factor_send, factor_in, factor_part, factor_out_s, factor_core,
    part, core_out, core_in, chip_acc, chip_out, chip_in,
    msub_acc, msub_out, msub_in, mwhole, sub_acc, sub_out, sub_in, whole,
    load_sem, fwd_send, fwd_recv, back_send, back_recv,
    known_send, known_recv, factor_ssem, factor_rsem, core_send, core_recv,
    mcore_send, mcore_recv, chip_send, chip_recv, msub_send, msub_recv,
    msubg_send, msubg_recv, mchipg_send, mchipg_recv, mcoreg_send, mcoreg_recv,
    sub_send, sub_recv,
    subg_send, subg_recv, chipg_send, chipg_recv, coreg_send, coreg_recv,
):
    g = lax.axis_index("grid")
    c = lax.axis_index("sub")
    core = lax.rem(g, 2)
    chip = lax.div(g, 2)
    chips = n_grid // 2
    other_core = g + 1 - 2 * core
    points, width = x_s.shape
    nodes = mesh_s.shape[0]
    slots_per = rows_s.shape[3]
    fanout = nbr_s.shape[1]
    heads = bias_s.shape[1] // fanout
    head = width // heads
    slots = 3 * n_sub * slots_per
    scale = head ** (-0.5)
    half = points // 2

    loads = {}
    pairs = (
        ("rows", rows, rows_s), ("x", grid_x, x_s), ("gg", gain_g, gg_s), ("nbr", nbr, nbr_s),
        ("bias", bias, bias_s), ("valid", valid, valid_s), ("mesh", mesh_h, mesh_s),
        ("gm", gain_m, gm_s), ("wq", w_q, wq_s), ("og", out_grad, og_s), ("wo", w_o, wo_s),
        ("wk", w_k, wk_s), ("wv", w_v, wv_s),
    )
    for at, (name, source, target) in enumerate(pairs):
        loads[name] = pltpu.make_async_copy(source, target, load_sem.at[at])
        loads[name].start()

    def wrap(value, size):
        return lax.rem(value + size, size)

    def remote(source, target, send, recv, to_grid, to_sub):
        return pltpu.make_async_remote_copy(
            src_ref=source, dst_ref=target, send_sem=send, recv_sem=recv,
            device_id={"grid": to_grid, "sub": to_sub}, device_id_type=pl.DeviceIdType.MESH,
        )

    barrier = pltpu.get_barrier_semaphore()
    peers = [
        (wrap(g + o, n_grid), wrap(c + k, n_sub))
        for k in range(n_sub) for o in (-1, 0, 1) if (o, k) != (0, 0)
    ] + [(lax.rem(chip + j, chips) * 2 + core, c) for j in range(1, chips)]
    for to_grid, to_sub in peers:
        pl.semaphore_signal(
            barrier, inc=1, device_id={"grid": to_grid, "sub": to_sub},
            device_id_type=pl.DeviceIdType.MESH,
        )

    far_first = sorted(range(n_sub), key=lambda k: -min(k, n_sub - k))

    loads["rows"].wait()
    eye = (
        lax.broadcasted_iota(jnp.int32, (slots_per, slots_per), 0)
        == lax.broadcasted_iota(jnp.int32, (slots_per, slots_per), 1)
    )
    forward = {}
    for o in (0, 2, 1):
        low, span = (0, half) if o == 0 else (half, points - half) if o == 2 else (0, points)
        lane = lax.broadcasted_iota(jnp.int32, (slots_per, span), 1) + low
        picks = []
        for s in range(n_sub):
            row = rows_s[0, o, pl.ds(s, 1), :].astype(F32)
            column = jnp.sum(jnp.where(eye, row, 0.0), axis=1, keepdims=True).astype(jnp.int32)
            picks.append(jnp.where(lane == column, 1.0, 0.0).astype(BF16))
        onehot = jnp.concatenate(picks, axis=0)
        if o == 0:
            loads["x"].wait()
            loads["gg"].wait()
        chosen = dot(onehot, x_s[pl.ds(low, span), :])
        factor = lax.rsqrt(jnp.mean(chosen * chosen, axis=-1, keepdims=True) + EPSILON)
        packet[o] = (chosen * factor * gg_s[...]).astype(BF16).reshape(n_sub, slots_per, width)
        if o == 0:
            pl.semaphore_wait(barrier, len(peers))
        for k in far_first:
            if (o, k) == (1, 0):
                continue
            to_sub = lax.rem(c + k, n_sub)
            forward[o, k] = remote(
                packet.at[o, to_sub], arrived.at[o, k],
                fwd_send.at[o * n_sub + k], fwd_recv.at[o * n_sub + k],
                wrap(g + o - 1, n_grid), to_sub,
            )
            forward[o, k].start()
    arrived[1, 0] = packet[1, c]

    for name in ("mesh", "gm", "og"):
        loads[name].wait()
    mesh_wide, mesh_factor, mesh_normed = normalize(mesh_s[...], gm_s[...])
    known[0, pl.ds(chip, 1)] = og_s[...][None]
    known[1, pl.ds(chip, 1)] = mesh_normed[None]
    known_moves = {}
    for ch in range(2):
        known_moves["known", ch] = []
        for j in range(1, chips):
            to_chip = lax.rem(chip + j, chips)
            move = remote(
                known.at[ch, chip], known.at[ch, chip], known_send.at[ch, j], known_recv.at[ch, j],
                to_chip * 2 + core, c,
            )
            move.start()
            known_moves["known", ch].append(move)

    for name in ("nbr", "bias", "valid"):
        loads[name].wait()
    named = nbr_s[...]
    offset_of = lax.div(named, n_sub * slots_per)
    sub_of = lax.rem(lax.div(named, slots_per), n_sub)
    turn = lax.rem(c - sub_of + n_sub, n_sub)
    slot_of[...] = (offset_of * n_sub + turn) * slots_per + lax.rem(named, slots_per)
    edge_rows[...] = jnp.zeros(edge_rows.shape, F32)
    for h in range(heads):
        values = bias_s[:, h * fanout:(h + 1) * fanout]
        high = values.astype(BF16).astype(F32)
        middle = (values - high).astype(BF16).astype(F32)
        edge_rows[pl.ds(h, nodes, stride=ROWS), :fanout] = high
        edge_rows[pl.ds(8 + h, nodes, stride=ROWS), :fanout] = middle
        edge_rows[pl.ds(16 + h, nodes, stride=ROWS), :fanout] = values - high - middle
    edge_rows[pl.ds(heads, nodes, stride=ROWS), :fanout] = jnp.where(valid_s[...] == 1, 1.0, 0.0)

    slot_ids = lax.broadcasted_iota(jnp.int32, (slots, fanout), 0)
    group = 8

    def spread(step, carry):
        for inner in range(group):
            node = step * group + inner
            names = slot_ids == slot_of[pl.ds(node, 1), :]
            onehot = jnp.where(names, 1.0, 0.0).astype(BF16)
            at = pl.multiple_of(node * ROWS, 8)
            spread_rows = dot(edge_rows[pl.ds(at, ROWS), :fanout].astype(BF16), onehot, NT)
            total = (spread_rows[16:24] + spread_rows[8:16]) + spread_rows[:8]
            for tile in range(slots // LANES):
                dense[tile, pl.ds(pl.multiple_of(node * 8, 8), 8), :] = (
                    total[:, tile * LANES:(tile + 1) * LANES]
                )
        return carry

    lax.fori_loop(0, nodes // group, spread, 0)

    for o in range(3):
        for s in range(n_sub):
            at = (o * n_sub + s) * slots_per
            flat[:, at:at + slots_per] = rows_s[0, o, pl.ds(s, 1), :]
    block_rows = n_sub * slots_per
    for h in range(2):
        point = lax.broadcasted_iota(jnp.int32, (half, 2 * block_rows), 0) + h * half
        names = point == flat[:, h * block_rows:(h + 2) * block_rows]
        onehot_t[h] = jnp.where(names, 1.0, 0.0).astype(BF16)
    tile = half // 2
    for b in range(4):
        wide = x_s[b * tile:(b + 1) * tile, :].astype(F32)
        factor_s[b * tile:(b + 1) * tile, :] = lax.rsqrt(
            jnp.mean(wide * wide, axis=-1, keepdims=True) + EPSILON
        )

    for name in ("wq", "wo", "wk", "wv"):
        loads[name].wait()
    q_s[...] = (dot(mesh_normed, wq_s[...]) * scale).astype(BF16)
    ag_s[...] = dot(og_s[...], wo_s[...], NT).astype(BF16)

    for o in (0, 2, 1):
        for k in range(n_sub):
            if (o, k) != (1, 0):
                forward[o, k].wait_recv()
        here = slice(o * n_sub * slots_per, (o + 1) * n_sub * slots_per)
        rows_in = arrived[o].reshape(n_sub * slots_per, width)
        rows_t[:, here] = rows_in.T
        k_s[here, :] = dot(rows_in, wk_s[...]).astype(BF16)
        v_s[here, :] = dot(rows_in, wv_s[...]).astype(BF16)

    def spread_of(row):
        return jnp.concatenate(
            [dense[tile, pl.ds(row, nodes, stride=8), :] for tile in range(slots // LANES)], axis=1
        )

    live = spread_of(heads) > 0.5
    for h in range(heads):
        mine = slice(h * head, (h + 1) * head)
        queries, keys, values, att_grad = q_s[:, mine], k_s[:, mine], v_s[:, mine], ag_s[:, mine]
        scores = dot(queries, keys, NT) + spread_of(h)
        peak = jnp.max(jnp.where(live, scores, NEG_FILL), axis=1, keepdims=True)
        terms = jnp.exp(jnp.where(live, scores - peak, NEG_FILL))
        probs = terms / jnp.sum(terms, axis=1, keepdims=True)
        probs_b = probs.astype(BF16)
        att_s[:, mine] = dot(probs_b, values).astype(BF16)
        prob_grads = dot(att_grad, values, NT)
        score_grads = (
            probs * (prob_grads - jnp.sum(probs * prob_grads, axis=1, keepdims=True))
        ).astype(BF16)
        qg_s[:, mine] = (dot(score_grads, keys) * scale).astype(BF16)
        back_k[:, mine] = dot(score_grads, queries, TN).astype(BF16)
        back_v[:, mine] = dot(probs_b, att_grad, TN).astype(BF16)

    backward = {}

    def turn_back(o):
        here = slice(o * n_sub * slots_per, (o + 1) * n_sub * slots_per)
        total = dot(back_k[here, :], wk_s[...], NT) + dot(back_v[here, :], wv_s[...], NT)
        slot_back[o] = total.astype(BF16).reshape(n_sub, slots_per, width)

    def send_home(o, k):
        backward[o, k] = remote(
            slot_back.at[o, k], returned.at[o, c],
            back_send.at[o * n_sub + k], back_recv.at[o * n_sub + k],
            wrap(g + 1 - o, n_grid), wrap(c - k, n_sub),
        )
        backward[o, k].start()

    half_rows = width // 2
    chunks = whole.shape[0]
    block = half_rows // chips
    lanes = width // n_sub
    chip_bits = chips.bit_length() - 1
    moves = {}

    def flip(index, bit):
        return index + bit - 2 * bit * lax.rem(lax.div(index, bit), 2)

    def reverse(index, bits):
        total = 0
        for t in range(bits):
            total = total + lax.rem(lax.div(index, 2**t), 2) * 2 ** (bits - 1 - t)
        return total

    chip_of = (chip, reverse(chip, chip_bits))

    def start(key, *move):
        moves.setdefault(key, []).append(remote(*move))
        moves[key][-1].start()

    def arrive(key):
        for move in moves[key]:
            move.wait_recv()

    def factor_out(ch):
        source = (att_s, qg_s)[ch]
        piece = width // chips
        for j in range(chips):
            factor_send[ch, j] = source[:, j * piece:(j + 1) * piece]
        for j in range(1, chips):
            to_chip = lax.rem(chip + j, chips)
            start(
                ("factor", ch), factor_send.at[ch, to_chip], factor_in.at[ch, chip],
                factor_ssem.at[ch, j], factor_rsem.at[ch, j], to_chip * 2 + core, c,
            )
        factor_in[ch, pl.ds(chip, 1)] = factor_send[ch, pl.ds(chip, 1)]

    def factor_sum(ch):
        arrive(("factor", ch))
        arrive(("known", ch))
        total = dot(
            factor_in[ch].reshape(chips * nodes, width // chips),
            known[ch].reshape(chips * nodes, width), TN,
        )
        factor_part[ch] = total.reshape(2, block, width)
        factor_out_s[ch] = factor_part[ch, 1 - core].astype(BF16)
        start(
            ("core", ch), factor_out_s.at[ch], factor_core.at[ch],
            core_send.at[ch], core_recv.at[ch], other_core, c,
        )

    quarter_rows = half_rows // 2
    part_rows = quarter_rows // chips
    thirds = [k for k in far_first if k]

    def core_stage(m, grad):
        part[m] = grad.reshape(2, quarter_rows, width)
        core_out[m] = part[m, 1 - core].astype(BF16)
        start(
            ("mcore", m), core_out.at[m], core_in.at[m],
            mcore_send.at[m], mcore_recv.at[m], other_core, c,
        )

    def chip_stage(m):
        arrive(("mcore", m))
        for j in range(chips):
            at = pl.ds(j * part_rows, part_rows)
            total = part[m, core, at, :] + core_in[m, at, :].astype(F32)
            chip_acc[m, j] = total
            chip_out[m, j] = total.astype(BF16)
        for j in range(1, chips):
            to_chip = lax.rem(chip + j, chips)
            start(
                ("mchip", m), chip_out.at[m, to_chip], chip_in.at[m, j],
                chip_send.at[m, j], chip_recv.at[m, j], to_chip * 2 + core, c,
            )

    def sub_stage(m):
        arrive(("mchip", m))
        total = chip_acc[m, chip]
        for j in range(1, chips):
            total = total + chip_in[m, j].astype(F32)
        for z in range(n_sub):
            piece = total[:, z * lanes:(z + 1) * lanes]
            msub_acc[m, z] = piece
            msub_out[m, z] = piece.astype(BF16)
        for k in thirds:
            to_sub = lax.rem(c + k, n_sub)
            start(
                ("msub", m), msub_out.at[m, to_sub], msub_in.at[m, k],
                msub_send.at[m, k], msub_recv.at[m, k], g, to_sub,
            )

    def sub_spread(m):
        arrive(("msub", m))
        total = msub_acc[m, c]
        for k in range(1, n_sub):
            total = total + msub_in[m, k].astype(F32)
        mwhole[m, chip, pl.ds(c, 1)] = total.astype(BF16)[None]
        piece = mwhole.at[m, chip, c]
        for k in thirds:
            start(
                ("msubg", m), piece, piece, msubg_send.at[m, k], msubg_recv.at[m, k],
                g, lax.rem(c + k, n_sub),
            )

    def chip_spread(m):
        arrive(("msubg", m))
        piece = mwhole.at[m, chip]
        for j in range(1, chips):
            start(
                ("mchipg", m), piece, piece, mchipg_send.at[m, j], mchipg_recv.at[m, j],
                lax.rem(chip + j, chips) * 2 + core, c,
            )

    def core_spread(m):
        arrive(("mchipg", m))
        start(
            ("mcoreg", m), mwhole.at[m], mgathered.at[m, core],
            mcoreg_send.at[m], mcoreg_recv.at[m], other_core, c,
        )
        mgathered[m, pl.ds(core, 1)] = mwhole[m][None]

    def sub_first(ch):
        arrive(("core", ch))
        total = factor_part[ch, core] + factor_core[ch].astype(F32)
        for z in range(n_sub):
            piece = total[:, z * lanes:(z + 1) * lanes]
            sub_acc[ch, z] = piece
            sub_out[ch, z] = piece.astype(BF16)
        for k in thirds:
            to_sub = lax.rem(c + k, n_sub)
            start(
                ("sub", ch), sub_out.at[ch, to_sub], sub_in.at[ch, k],
                sub_send.at[ch, k], sub_recv.at[ch, k], g, to_sub,
            )

    def sub_gather(ch):
        arrive(("sub", ch))
        total = sub_acc[ch, c]
        for k in range(1, n_sub):
            total = total + sub_in[ch, k].astype(F32)
        p = lax.div(c, n_sub // 2)
        at_chip = chip_of[0] * (1 - p) + chip_of[1] * p
        spot = lax.rem(c, n_sub // 2)
        whole[ch, p, at_chip, pl.ds(spot, 1)] = total.astype(BF16)[None]
        piece = whole.at[ch, p, at_chip, spot]
        for k in thirds:
            start(
                ("subg", ch), piece, piece, subg_send.at[ch, k], subg_recv.at[ch, k],
                g, lax.rem(c + k, n_sub),
            )

    def chip_step(ch, t):
        for p in range(2):
            bit = 2**t if p == 0 else 2 ** (chip_bits - 1 - t)
            low = lax.div(chip_of[p], 2**t) * 2**t
            piece = whole.at[ch, p, pl.ds(low, 2**t)]
            start(
                ("chipg", ch, t), piece, piece, chipg_send.at[ch, p, t], chipg_recv.at[ch, p, t],
                flip(chip, bit) * 2 + core, c,
            )

    def chip_gather(ch):
        arrive(("subg", ch))
        chip_step(ch, 0)

    def chip_gather_next(ch):
        for t in range(1, chip_bits):
            arrive(("chipg", ch, t - 1))
            chip_step(ch, t)

    def core_gather(ch):
        arrive(("chipg", ch, chip_bits - 1))
        start(
            ("coreg", ch), whole.at[ch], gathered.at[ch, core],
            coreg_send.at[ch], coreg_recv.at[ch], other_core, c,
        )
        gathered[ch, pl.ds(core, 1)] = whole[ch][None]

    moves.update(known_moves)
    home = [(o, k) for o in (0, 2, 1) for k in far_first if (o, k) != (1, 0)]

    def send_next(count=1):
        for _ in range(min(count, len(home))):
            send_home(*home.pop(0))

    def nodes_out():
        mo_s[...] = (mesh_wide + dot(att_s[...], wo_s[...])).astype(BF16)
        mesh_normed_grad = dot(qg_s[...], wq_s[...], NT)
        mg_s[...] = (
            og_s[...].astype(F32)
            + normalize_back(mesh_wide, mesh_factor, gm_s[...], mesh_normed_grad)
        ).astype(BF16)

    def stage_of_matrix(m):
        span = slice(m % 2 * half_rows, (m % 2 + 1) * half_rows)
        core_stage(m, dot(rows_t[span, :], (back_k, back_v)[m // 2][...]))

    for stage, *of in (
        (factor_out, 0), (factor_out, 1), (turn_back, 0), (send_next, 3),
        (stage_of_matrix, 0), (stage_of_matrix, 1), (stage_of_matrix, 2), (stage_of_matrix, 3),
        (factor_sum, 0), (factor_sum, 1),
        (chip_stage, 0), (chip_stage, 1), (chip_stage, 2), (chip_stage, 3),
        (sub_first, 0), (sub_first, 1), (turn_back, 2), (send_next, 3), (turn_back, 1), (nodes_out,),
        (sub_gather, 0), (sub_gather, 1),
        (sub_stage, 0), (sub_stage, 1), (sub_stage, 2), (sub_spread, 0),
        (chip_gather, 0), (chip_gather, 1),
        (sub_stage, 3), (sub_spread, 1), (sub_spread, 2), (sub_spread, 3), (send_next, 1),
        (chip_gather_next, 0), (chip_gather_next, 1), (send_next, 1),
        (chip_spread, 0), (chip_spread, 1), (send_next, 1),
        (chip_spread, 2), (chip_spread, 3), (send_next, 2),
        (core_gather, 0), (core_gather, 1),
        (core_spread, 0), (core_spread, 1), (core_spread, 2), (core_spread, 3),
    ):
        stage(*of)
    returned[1, pl.ds(c, 1)] = slot_back[1, 0][None]
    send_next(len(home))
    for move in backward.values():
        move.wait_recv()
    for b in range(4):
        h, at = b // 2, slice(b * tile, (b + 1) * tile)
        home_rows = returned[h:h + 2].reshape(2 * block_rows, width)
        normed_grad = dot(onehot_t[h, b % 2 * tile:(b % 2 + 1) * tile, :], home_rows)
        wide = x_s[at, :].astype(F32)
        grid_grad[at, :] = normalize_back(
            wide, factor_s[at, :], gg_s[...], normed_grad
        ).astype(BF16)
    for ch in range(chunks):
        arrive(("coreg", ch))
    for m in range(4):
        arrive(("mcoreg", m))
    for move in [*forward.values(), *backward.values()] + sum(moves.values(), []):
        move.wait_send()


def finish(
    gathered_s, mgathered_s, mo_s, mg_s, gx_s, mesh_out, mesh_grad, grid_grad, weight_grads,
    w_s, store_sem,
):
    width = gx_s.shape[1]
    half_rows = width // 2
    chunks, _, _, chips, halves, part_rows, part_lanes = gathered_s.shape
    n_sub = 2 * halves
    stores = []

    def store(source, target):
        move = pltpu.make_async_copy(source, target, store_sem.at[len(stores)])
        move.start()
        stores.append(move)

    store(gx_s, grid_grad)
    store(mo_s, mesh_out)
    store(mg_s, mesh_grad)
    chip_bits = chips.bit_length() - 1

    def flipped(index, bits):
        return sum((index >> t & 1) << (bits - 1 - t) for t in range(bits))

    def piece_of(ch, core, j, z):
        part, at = divmod(z, n_sub // 2)
        return gathered_s[ch, core, part, flipped(j, chip_bits) if part else j, at].astype(F32)

    for ch, matrix in enumerate((3, 0)):
        for j in range(chips):
            for z in range(n_sub):
                columns = slice(z * part_lanes, (z + 1) * part_lanes)
                span = slice(2 * j * part_rows, 2 * (j + 1) * part_rows)
                both = jnp.concatenate([piece_of(ch, core, j, z) for core in range(2)], axis=0)
                if ch == 0:
                    w_s[matrix, span, columns] = both
                else:
                    w_s[matrix, columns, span] = both.T
        store(w_s.at[matrix], weight_grads.at[matrix])
    for m in range(4):
        rows_of = part_rows // 2
        for core in range(2):
            for j in range(chips):
                at = m % 2 * half_rows + core * half_rows // 2 + j * rows_of
                for z in range(n_sub):
                    columns = slice(z * part_lanes, (z + 1) * part_lanes)
                    w_s[1 + m // 2, at:at + rows_of, columns] = mgathered_s[m, core, j, z].astype(F32)
        at = pl.ds(m % 2 * half_rows, half_rows)
        store(w_s.at[1 + m // 2, at], weight_grads.at[1 + m // 2, at])
    for move in stores:
        move.wait()


def shards(
    n_grid, n_sub,
    grid_x, mesh_h, gain_grid, gain_mesh, w_query, w_key, w_value, w_out,
    edge_bias, neighbours, valid, send_rows, out_grad,
):
    points, width = grid_x.shape
    nodes = mesh_h.shape[0]
    slots_per = send_rows.shape[3]
    fanout = neighbours.shape[1]
    slots = 3 * n_sub * slots_per
    chips = n_grid // 2
    chunks = 2
    half_rows = width // 2
    block, lanes = half_rows // chips, width // n_sub
    anywhere = pl.BlockSpec(memory_space=pl.ANY)
    inside = pl.BlockSpec(memory_space=pltpu.VMEM)
    dma = pltpu.SemaphoreType.DMA
    gain_grid, gain_mesh = gain_grid.reshape(1, width), gain_mesh.reshape(1, width)
    operands = (
        grid_x, mesh_h, gain_grid, gain_mesh, w_query, w_key, w_value, w_out,
        edge_bias, neighbours, valid, send_rows, out_grad,
    )
    blocks = (3, n_sub, slots_per, width)
    node_rows = pltpu.VMEM((nodes, width), BF16)
    slot_rows = pltpu.VMEM((slots, width), BF16)
    chip_bits = chips.bit_length() - 1
    pieces = (chunks, 2, 2, chips, n_sub // 2, block, lanes)
    mpieces = (4, 2, chips, n_sub, block // 2, lanes)
    kept = 2 * (points * width + 2 * nodes * width + 4 * width * width) + 2**16
    found = pl.pallas_call(
        functools.partial(layer, n_grid, n_sub),
        in_specs=[anywhere] * len(operands),
        out_specs=[inside] * 5,
        out_shape=[
            pltpu.VMEM((points, width), BF16),
            pltpu.VMEM(pieces, BF16),
            pltpu.VMEM(mpieces, BF16),
            node_rows, node_rows,
        ],
        scratch_shapes=[pltpu.VMEM(a.shape, a.dtype) for a in operands] + [
            pltpu.VMEM(blocks, BF16), pltpu.VMEM(blocks, BF16), pltpu.VMEM((width, slots), BF16),
            pltpu.VMEM(blocks, BF16), pltpu.VMEM(blocks, BF16), pltpu.VMEM((1, slots), jnp.int32),
            pltpu.VMEM((2, points // 2, 2 * n_sub * slots_per), BF16), pltpu.VMEM((points, 1), F32),
            pltpu.VMEM((nodes * ROWS, LANES), F32),
            pltpu.VMEM((slots // LANES, nodes * 8, LANES), F32),
            pltpu.VMEM((nodes, fanout), jnp.int32),
            node_rows, node_rows, slot_rows, slot_rows, node_rows, node_rows,
            slot_rows, slot_rows,
            pltpu.VMEM((2, chips, nodes, width), BF16),
            pltpu.VMEM((2, chips, nodes, width // chips), BF16),
            pltpu.VMEM((2, chips, nodes, width // chips), BF16),
            pltpu.VMEM((2, 2, block, width), F32),
            pltpu.VMEM((2, block, width), BF16), pltpu.VMEM((2, block, width), BF16),
            pltpu.VMEM((4, 2, half_rows // 2, width), F32),
            pltpu.VMEM((4, half_rows // 2, width), BF16), pltpu.VMEM((4, half_rows // 2, width), BF16),
            pltpu.VMEM((4, chips, block // 2, width), F32),
            pltpu.VMEM((4, chips, block // 2, width), BF16),
            pltpu.VMEM((4, chips, block // 2, width), BF16),
            pltpu.VMEM((4, n_sub, block // 2, lanes), F32),
            pltpu.VMEM((4, n_sub, block // 2, lanes), BF16),
            pltpu.VMEM((4, n_sub, block // 2, lanes), BF16),
            pltpu.VMEM(mpieces[:1] + mpieces[2:], BF16),
            pltpu.VMEM((chunks, n_sub, block, lanes), F32),
            pltpu.VMEM((chunks, n_sub, block, lanes), BF16),
            pltpu.VMEM((chunks, n_sub, block, lanes), BF16),
            pltpu.VMEM(pieces[:1] + pieces[2:], BF16),
            dma((len(operands),)),
            dma((3 * n_sub,)), dma((3 * n_sub,)), dma((3 * n_sub,)), dma((3 * n_sub,)),
            dma((2, chips)), dma((2, chips)), dma((2, chips)), dma((2, chips)),
            dma((chunks,)), dma((chunks,)),
            dma((4,)), dma((4,)), dma((4, chips)), dma((4, chips)), dma((4, n_sub)), dma((4, n_sub)),
            dma((4, n_sub)), dma((4, n_sub)), dma((4, chips)), dma((4, chips)), dma((4,)), dma((4,)),
            dma((chunks, n_sub)), dma((chunks, n_sub)),
            dma((chunks, n_sub)), dma((chunks, n_sub)),
            dma((chunks, 2, chip_bits)), dma((chunks, 2, chip_bits)),
            dma((chunks,)), dma((chunks,)),
        ],
        compiler_params=pltpu.CompilerParams(
            collective_id=0, has_side_effects=True, vmem_limit_bytes=VMEM_BYTES - kept
        ),
        name="layer",
    )(*operands)
    gx, gathered, mgathered, mo, mg = found
    return pl.pallas_call(
        finish,
        in_specs=[inside] * 5,
        out_specs=[anywhere] * 4,
        out_shape=[
            jax.ShapeDtypeStruct((nodes, width), BF16),
            jax.ShapeDtypeStruct((nodes, width), BF16),
            jax.ShapeDtypeStruct((points, width), BF16),
            jax.ShapeDtypeStruct((4, width, width), F32),
        ],
        scratch_shapes=[pltpu.VMEM((4, width, width), F32), dma((9,))],
        compiler_params=pltpu.CompilerParams(vmem_limit_bytes=LIMIT),
        name="finish",
    )(gathered, mgathered, mo, mg, gx)


def solution(mesh):
    by_device = P(("grid", "sub"), None)
    in_specs = (
        by_device, by_device, P(), P(), P(), P(), P(), P(), by_device, by_device, by_device,
        P(("grid", "sub"), None, None, None), by_device,
    )
    out_specs = (by_device, by_device, by_device, P())
    body = functools.partial(shards, mesh.shape["grid"], mesh.shape["sub"])
    return jax.shard_map(body, mesh=mesh, in_specs=in_specs, out_specs=out_specs, check_vma=False)
```

```python
import functools

import jax
import jax.numpy as jnp
from jax import lax
from jax.experimental import pallas as pl
from jax.experimental.pallas import tpu as pltpu
from jax.sharding import PartitionSpec as P

EPSILON = 1e-06
NEG_FILL = -1e30
F32 = jnp.float32
BF16 = jnp.bfloat16
NN = (((1,), (0,)), ((), ()))
NT = (((1,), (1,)), ((), ()))
TN = (((0,), (0,)), ((), ()))
LANES = 128
LIMIT = 32 * 2**20
VMEM_BYTES = 67043328
ROWS = 24


def dot(a, b, dims=NN):
    return lax.dot_general(a, b, dims, preferred_element_type=F32)


def normalize(values_in, gain_row):
    widened = values_in.astype(F32)
    factor = lax.rsqrt(jnp.mean(widened * widened, axis=-1, keepdims=True) + EPSILON)
    return (widened, factor, (widened * factor * gain_row).astype(BF16))


def normalize_back(widened, factor, gain_row, upstream):
    scaled = gain_row * upstream
    inner_mean = jnp.mean(widened * scaled, axis=-1, keepdims=True)
    return factor * scaled - widened * factor**3 * inner_mean


def layer(
    n_grid,
    n_sub,
    grid_x, mesh_h, gain_g, gain_m, w_q, w_k, w_v, w_o, bias, nbr, valid, rows, out_grad,
    grid_grad, gathered, mgathered, mo_s, mg_s,
    x_s, mesh_s, gg_s, gm_s, wq_s, wk_s, wv_s, wo_s, bias_s, nbr_s, valid_s, rows_s, og_s,
    packet, arrived, rows_t, slot_back, returned, flat, onehot_t, factor_s,
    edge_rows, dense, slot_of, q_s, ag_s, k_s, v_s, att_s, qg_s, back_k, back_v,
    known, factor_send, factor_in, factor_part, factor_out_s, factor_core,
    part, core_out, core_in, chip_acc, chip_out, chip_in,
    msub_acc, msub_out, msub_in, mwhole, sub_acc, sub_out, sub_in, whole,
    load_sem, fwd_send, fwd_recv, back_send, back_recv,
    known_send, known_recv, factor_ssem, factor_rsem, core_send, core_recv,
    mcore_send, mcore_recv, chip_send, chip_recv, msub_send, msub_recv,
    msubg_send, msubg_recv, mchipg_send, mchipg_recv, mcoreg_send, mcoreg_recv,
    sub_send, sub_recv,
    subg_send, subg_recv, chipg_send, chipg_recv, coreg_send, coreg_recv,
):
    g = lax.axis_index("grid")
    c = lax.axis_index("sub")
    core = lax.rem(g, 2)
    chip = lax.div(g, 2)
    chips = n_grid // 2
    other_core = g + 1 - 2 * core
    points, width = x_s.shape
    nodes = mesh_s.shape[0]
    slots_per = rows_s.shape[3]
    fanout = nbr_s.shape[1]
    heads = bias_s.shape[1] // fanout
    head = width // heads
    slots = 3 * n_sub * slots_per
    scale = head ** (-0.5)
    half = points // 2

    def wrap(value, size):
        return lax.rem(value + size, size)

    def remote(source, target, send, recv, to_grid, to_sub):
        return pltpu.make_async_remote_copy(
            src_ref=source, dst_ref=target, send_sem=send, recv_sem=recv,
            device_id={"grid": to_grid, "sub": to_sub}, device_id_type=pl.DeviceIdType.MESH,
        )

    barrier = pltpu.get_barrier_semaphore()
    peers = [
        (wrap(g + o, n_grid), wrap(c + k, n_sub))
        for k in range(n_sub) for o in (-1, 0, 1) if (o, k) != (0, 0)
    ] + [(lax.rem(chip + j, chips) * 2 + core, c) for j in range(1, chips)]
    for to_grid, to_sub in peers:
        pl.semaphore_signal(
            barrier, inc=1, device_id={"grid": to_grid, "sub": to_sub},
            device_id_type=pl.DeviceIdType.MESH,
        )

    loads = {}
    pairs = (
        ("rows", rows, rows_s), ("x", grid_x, x_s), ("gg", gain_g, gg_s), ("nbr", nbr, nbr_s),
        ("bias", bias, bias_s), ("valid", valid, valid_s), ("mesh", mesh_h, mesh_s),
        ("gm", gain_m, gm_s), ("wq", w_q, wq_s), ("og", out_grad, og_s), ("wo", w_o, wo_s),
        ("wk", w_k, wk_s), ("wv", w_v, wv_s),
    )
    for at, (name, source, target) in enumerate(pairs):
        loads[name] = pltpu.make_async_copy(source, target, load_sem.at[at])
        loads[name].start()

    far_first = sorted(range(n_sub), key=lambda k: -min(k, n_sub - k))

    loads["rows"].wait()
    eye = (
        lax.broadcasted_iota(jnp.int32, (slots_per, slots_per), 0)
        == lax.broadcasted_iota(jnp.int32, (slots_per, slots_per), 1)
    )
    forward = {}
    for o in (0, 2, 1):
        low, span = (0, half) if o == 0 else (half, points - half) if o == 2 else (0, points)
        lane = lax.broadcasted_iota(jnp.int32, (slots_per, span), 1) + low
        picks = []
        for s in range(n_sub):
            row = rows_s[0, o, pl.ds(s, 1), :].astype(F32)
            column = jnp.sum(jnp.where(eye, row, 0.0), axis=1, keepdims=True).astype(jnp.int32)
            picks.append(jnp.where(lane == column, 1.0, 0.0).astype(BF16))
        onehot = jnp.concatenate(picks, axis=0)
        if o == 0:
            loads["x"].wait()
            loads["gg"].wait()
        chosen = dot(onehot, x_s[pl.ds(low, span), :])
        factor = lax.rsqrt(jnp.mean(chosen * chosen, axis=-1, keepdims=True) + EPSILON)
        packet[o] = (chosen * factor * gg_s[...]).astype(BF16).reshape(n_sub, slots_per, width)
        if o == 0:
            pl.semaphore_wait(barrier, len(peers))
        for k in far_first:
            if (o, k) == (1, 0):
                continue
            to_sub = lax.rem(c + k, n_sub)
            forward[o, k] = remote(
                packet.at[o, to_sub], arrived.at[o, k],
                fwd_send.at[o * n_sub + k], fwd_recv.at[o * n_sub + k],
                wrap(g + o - 1, n_grid), to_sub,
            )
            forward[o, k].start()
    arrived[1, 0] = packet[1, c]

    for name in ("mesh", "gm", "og"):
        loads[name].wait()
    mesh_wide, mesh_factor, mesh_normed = normalize(mesh_s[...], gm_s[...])
    known[0, pl.ds(chip, 1)] = og_s[...][None]
    known[1, pl.ds(chip, 1)] = mesh_normed[None]
    known_moves = {}
    for ch in range(2):
        known_moves["known", ch] = []
        for j in range(1, chips):
            to_chip = lax.rem(chip + j, chips)
            move = remote(
                known.at[ch, chip], known.at[ch, chip], known_send.at[ch, j], known_recv.at[ch, j],
                to_chip * 2 + core, c,
            )
            move.start()
            known_moves["known", ch].append(move)

    for name in ("nbr", "bias", "valid"):
        loads[name].wait()
    named = nbr_s[...]
    offset_of = lax.div(named, n_sub * slots_per)
    sub_of = lax.rem(lax.div(named, slots_per), n_sub)
    turn = lax.rem(c - sub_of + n_sub, n_sub)
    slot_of[...] = (offset_of * n_sub + turn) * slots_per + lax.rem(named, slots_per)
    edge_rows[...] = jnp.zeros(edge_rows.shape, F32)
    for h in range(heads):
        values = bias_s[:, h * fanout:(h + 1) * fanout]
        high = values.astype(BF16).astype(F32)
        middle = (values - high).astype(BF16).astype(F32)
        edge_rows[pl.ds(h, nodes, stride=ROWS), :fanout] = high
        edge_rows[pl.ds(8 + h, nodes, stride=ROWS), :fanout] = middle
        edge_rows[pl.ds(16 + h, nodes, stride=ROWS), :fanout] = values - high - middle
    edge_rows[pl.ds(heads, nodes, stride=ROWS), :fanout] = jnp.where(valid_s[...] == 1, 1.0, 0.0)

    slot_ids = lax.broadcasted_iota(jnp.int32, (slots, fanout), 0)
    group = 8

    def spread(step, carry):
        for inner in range(group):
            node = step * group + inner
            names = slot_ids == slot_of[pl.ds(node, 1), :]
            onehot = jnp.where(names, 1.0, 0.0).astype(BF16)
            at = pl.multiple_of(node * ROWS, 8)
            spread_rows = dot(edge_rows[pl.ds(at, ROWS), :fanout].astype(BF16), onehot, NT)
            total = (spread_rows[16:24] + spread_rows[8:16]) + spread_rows[:8]
            for tile in range(slots // LANES):
                dense[tile, pl.ds(pl.multiple_of(node * 8, 8), 8), :] = (
                    total[:, tile * LANES:(tile + 1) * LANES]
                )
        return carry

    lax.fori_loop(0, nodes // group, spread, 0)

    for o in range(3):
        for s in range(n_sub):
            at = (o * n_sub + s) * slots_per
            flat[:, at:at + slots_per] = rows_s[0, o, pl.ds(s, 1), :]
    block_rows = n_sub * slots_per
    for h in range(2):
        point = lax.broadcasted_iota(jnp.int32, (half, 2 * block_rows), 0) + h * half
        names = point == flat[:, h * block_rows:(h + 2) * block_rows]
        onehot_t[h] = jnp.where(names, 1.0, 0.0).astype(BF16)
    tile = half // 2
    for b in range(4):
        wide = x_s[b * tile:(b + 1) * tile, :].astype(F32)
        factor_s[b * tile:(b + 1) * tile, :] = lax.rsqrt(
            jnp.mean(wide * wide, axis=-1, keepdims=True) + EPSILON
        )

    for name in ("wq", "wo", "wk", "wv"):
        loads[name].wait()
    q_s[...] = (dot(mesh_normed, wq_s[...]) * scale).astype(BF16)
    ag_s[...] = dot(og_s[...], wo_s[...], NT).astype(BF16)

    for o in (0, 2, 1):
        for k in range(n_sub):
            if (o, k) != (1, 0):
                forward[o, k].wait_recv()
        here = slice(o * n_sub * slots_per, (o + 1) * n_sub * slots_per)
        rows_in = arrived[o].reshape(n_sub * slots_per, width)
        rows_t[:, here] = rows_in.T
        k_s[here, :] = dot(rows_in, wk_s[...]).astype(BF16)
        v_s[here, :] = dot(rows_in, wv_s[...]).astype(BF16)

    def spread_of(row):
        return jnp.concatenate(
            [dense[tile, pl.ds(row, nodes, stride=8), :] for tile in range(slots // LANES)], axis=1
        )

    live = spread_of(heads) > 0.5
    for h in range(heads):
        mine = slice(h * head, (h + 1) * head)
        queries, keys, values, att_grad = q_s[:, mine], k_s[:, mine], v_s[:, mine], ag_s[:, mine]
        scores = dot(queries, keys, NT) + spread_of(h)
        peak = jnp.max(jnp.where(live, scores, NEG_FILL), axis=1, keepdims=True)
        terms = jnp.exp(jnp.where(live, scores - peak, NEG_FILL))
        probs = terms / jnp.sum(terms, axis=1, keepdims=True)
        probs_b = probs.astype(BF16)
        att_s[:, mine] = dot(probs_b, values).astype(BF16)
        prob_grads = dot(att_grad, values, NT)
        score_grads = (
            probs * (prob_grads - jnp.sum(probs * prob_grads, axis=1, keepdims=True))
        ).astype(BF16)
        qg_s[:, mine] = (dot(score_grads, keys) * scale).astype(BF16)
        back_k[:, mine] = dot(score_grads, queries, TN).astype(BF16)
        back_v[:, mine] = dot(probs_b, att_grad, TN).astype(BF16)

    backward = {}

    def turn_back(o):
        here = slice(o * n_sub * slots_per, (o + 1) * n_sub * slots_per)
        total = dot(back_k[here, :], wk_s[...], NT) + dot(back_v[here, :], wv_s[...], NT)
        slot_back[o] = total.astype(BF16).reshape(n_sub, slots_per, width)
        if o == 1:
            returned[1, pl.ds(c, 1)] = slot_back[1, 0][None]

    def send_home(o, k):
        backward[o, k] = remote(
            slot_back.at[o, k], returned.at[o, c],
            back_send.at[o * n_sub + k], back_recv.at[o * n_sub + k],
            wrap(g + 1 - o, n_grid), wrap(c - k, n_sub),
        )
        backward[o, k].start()

    half_rows = width // 2
    chunks = whole.shape[0]
    block = half_rows // chips
    lanes = width // n_sub
    chip_bits = chips.bit_length() - 1
    moves = {}

    def reverse(index, bits):
        total = 0
        for t in range(bits):
            total = total + lax.rem(lax.div(index, 2**t), 2) * 2 ** (bits - 1 - t)
        return total

    chip_of = (chip, reverse(chip, chip_bits))

    def start(key, *move):
        moves.setdefault(key, []).append(remote(*move))
        moves[key][-1].start()

    def arrive(key):
        for move in moves[key]:
            move.wait_recv()

    def factor_out(ch):
        source = (att_s, qg_s)[ch]
        piece = width // chips
        for j in range(chips):
            factor_send[ch, j] = source[:, j * piece:(j + 1) * piece]
        for j in range(1, chips):
            to_chip = lax.rem(chip + j, chips)
            start(
                ("factor", ch), factor_send.at[ch, to_chip], factor_in.at[ch, chip],
                factor_ssem.at[ch, j], factor_rsem.at[ch, j], to_chip * 2 + core, c,
            )
        factor_in[ch, pl.ds(chip, 1)] = factor_send[ch, pl.ds(chip, 1)]

    def factor_sum(ch):
        arrive(("factor", ch))
        arrive(("known", ch))
        total = dot(
            factor_in[ch].reshape(chips * nodes, width // chips),
            known[ch].reshape(chips * nodes, width), TN,
        )
        factor_part[ch] = total.reshape(2, block, width)
        factor_out_s[ch] = factor_part[ch, 1 - core].astype(BF16)
        start(
            ("core", ch), factor_out_s.at[ch], factor_core.at[ch],
            core_send.at[ch], core_recv.at[ch], other_core, c,
        )

    quarter_rows = half_rows // 2
    part_rows = quarter_rows // chips
    thirds = [k for k in far_first if k]

    def core_stage(m, grad):
        part[m] = grad.reshape(2, quarter_rows, width)
        core_out[m] = part[m, 1 - core].astype(BF16)
        start(
            ("mcore", m), core_out.at[m], core_in.at[m],
            mcore_send.at[m], mcore_recv.at[m], other_core, c,
        )

    def chip_stage(m):
        arrive(("mcore", m))
        for j in range(chips):
            at = pl.ds(j * part_rows, part_rows)
            total = part[m, core, at, :] + core_in[m, at, :].astype(F32)
            chip_acc[m, j] = total
            chip_out[m, j] = total.astype(BF16)
        for j in range(1, chips):
            to_chip = lax.rem(chip + j, chips)
            start(
                ("mchip", m), chip_out.at[m, to_chip], chip_in.at[m, j],
                chip_send.at[m, j], chip_recv.at[m, j], to_chip * 2 + core, c,
            )

    def sub_stage(m):
        arrive(("mchip", m))
        total = chip_acc[m, chip]
        for j in range(1, chips):
            total = total + chip_in[m, j].astype(F32)
        for z in range(n_sub):
            piece = total[:, z * lanes:(z + 1) * lanes]
            msub_acc[m, z] = piece
            msub_out[m, z] = piece.astype(BF16)
        for k in thirds:
            to_sub = lax.rem(c + k, n_sub)
            start(
                ("msub", m), msub_out.at[m, to_sub], msub_in.at[m, k],
                msub_send.at[m, k], msub_recv.at[m, k], g, to_sub,
            )

    def sub_spread(m):
        arrive(("msub", m))
        total = msub_acc[m, c]
        for k in range(1, n_sub):
            total = total + msub_in[m, k].astype(F32)
        mwhole[m, chip, pl.ds(c, 1)] = total.astype(BF16)[None]
        piece = mwhole.at[m, chip, c]
        for k in thirds:
            start(
                ("msubg", m), piece, piece, msubg_send.at[m, k], msubg_recv.at[m, k],
                g, lax.rem(c + k, n_sub),
            )

    def chip_spread(m):
        arrive(("msubg", m))
        piece = mwhole.at[m, chip]
        for j in range(1, chips):
            start(
                ("mchipg", m), piece, piece, mchipg_send.at[m, j], mchipg_recv.at[m, j],
                lax.rem(chip + j, chips) * 2 + core, c,
            )

    def core_spread(m):
        arrive(("mchipg", m))
        start(
            ("mcoreg", m), mwhole.at[m], mgathered.at[m, core],
            mcoreg_send.at[m], mcoreg_recv.at[m], other_core, c,
        )
        mgathered[m, pl.ds(core, 1)] = mwhole[m][None]

    def sub_first(ch):
        arrive(("core", ch))
        total = factor_part[ch, core] + factor_core[ch].astype(F32)
        for z in range(n_sub):
            piece = total[:, z * lanes:(z + 1) * lanes]
            sub_acc[ch, z] = piece
            sub_out[ch, z] = piece.astype(BF16)
        for k in thirds:
            to_sub = lax.rem(c + k, n_sub)
            start(
                ("sub", ch), sub_out.at[ch, to_sub], sub_in.at[ch, k],
                sub_send.at[ch, k], sub_recv.at[ch, k], g, to_sub,
            )

    def sub_gather(ch):
        arrive(("sub", ch))
        total = sub_acc[ch, c]
        for k in range(1, n_sub):
            total = total + sub_in[ch, k].astype(F32)
        p = lax.div(c, n_sub // 2)
        at_chip = chip_of[0] * (1 - p) + chip_of[1] * p
        spot = lax.rem(c, n_sub // 2)
        whole[ch, p, at_chip, pl.ds(spot, 1)] = total.astype(BF16)[None]
        piece = whole.at[ch, p, at_chip, spot]
        for k in thirds:
            start(
                ("subg", ch), piece, piece, subg_send.at[ch, k], subg_recv.at[ch, k],
                g, lax.rem(c + k, n_sub),
            )

    def chip_gather(ch):
        arrive(("subg", ch))
        for p in range(2):
            piece = whole.at[ch, p, chip_of[p]]
            for j in range(1, chips):
                start(
                    ("chipg", ch), piece, piece, chipg_send.at[ch, p, j], chipg_recv.at[ch, p, j],
                    lax.rem(chip + j, chips) * 2 + core, c,
                )

    def core_gather(ch):
        arrive(("chipg", ch))
        start(
            ("coreg", ch), whole.at[ch], gathered.at[ch, core],
            coreg_send.at[ch], coreg_recv.at[ch], other_core, c,
        )
        gathered[ch, pl.ds(core, 1)] = whole[ch][None]

    moves.update(known_moves)
    home = [(o, k) for o in (0, 2, 1) for k in far_first if (o, k) != (1, 0)]

    def send_next(count=1):
        for _ in range(min(count, len(home))):
            send_home(*home.pop(0))

    def nodes_out():
        mo_s[...] = (mesh_wide + dot(att_s[...], wo_s[...])).astype(BF16)
        mesh_normed_grad = dot(qg_s[...], wq_s[...], NT)
        mg_s[...] = (
            og_s[...].astype(F32)
            + normalize_back(mesh_wide, mesh_factor, gm_s[...], mesh_normed_grad)
        ).astype(BF16)

    def grid_rows(b):
        if b == 0:
            for move in backward.values():
                move.wait_recv()
        h, at = b // 2, slice(b * tile, (b + 1) * tile)
        home_rows = returned[h:h + 2].reshape(2 * block_rows, width)
        normed_grad = dot(onehot_t[h, b % 2 * tile:(b % 2 + 1) * tile, :], home_rows)
        wide = x_s[at, :].astype(F32)
        grid_grad[at, :] = normalize_back(
            wide, factor_s[at, :], gg_s[...], normed_grad
        ).astype(BF16)

    def stage_of_matrix(m):
        span = slice(m % 2 * half_rows, (m % 2 + 1) * half_rows)
        core_stage(m, dot(rows_t[span, :], (back_k, back_v)[m // 2][...]))

    for stage, *of in (
        (factor_out, 0), (factor_out, 1), (turn_back, 0), (send_next, 3), (stage_of_matrix, 0),
        (stage_of_matrix, 1), (stage_of_matrix, 2), (stage_of_matrix, 3), (factor_sum, 0),
        (factor_sum, 1), (chip_stage, 0), (chip_stage, 1), (chip_stage, 2), (chip_stage, 3),
        (sub_first, 0), (sub_first, 1), (turn_back, 2), (send_next, 1), (turn_back, 1),
        (nodes_out,), (sub_gather, 0), (sub_gather, 1), (sub_stage, 0), (sub_stage, 1),
        (sub_stage, 2), (sub_stage, 3), (send_next, 1), (chip_gather, 0), (chip_gather, 1),
        (sub_spread, 0), (send_next, 1), (sub_spread, 1), (send_next, 1), (sub_spread, 2),
        (send_next, 1), (sub_spread, 3), (send_next, 3), (chip_spread, 0), (chip_spread, 1),
        (chip_spread, 2), (chip_spread, 3), (core_gather, 0), (core_gather, 1), (grid_rows, 0),
        (grid_rows, 1), (grid_rows, 2), (grid_rows, 3), (core_spread, 0), (core_spread, 1),
        (core_spread, 2), (core_spread, 3),
    ):
        stage(*of)
    for ch in range(chunks):
        arrive(("coreg", ch))
    for m in range(4):
        arrive(("mcoreg", m))
    for move in [*forward.values(), *backward.values()] + sum(moves.values(), []):
        move.wait_send()


def finish(
    gathered_s, mgathered_s, mo_s, mg_s, gx_s, mesh_out, mesh_grad, grid_grad, weight_grads,
    w_s, store_sem,
):
    width = gx_s.shape[1]
    half_rows = width // 2
    chunks, _, _, chips, halves, part_rows, part_lanes = gathered_s.shape
    n_sub = 2 * halves
    stores = []

    def store(source, target):
        move = pltpu.make_async_copy(source, target, store_sem.at[len(stores)])
        move.start()
        stores.append(move)

    store(gx_s, grid_grad)
    store(mo_s, mesh_out)
    store(mg_s, mesh_grad)
    chip_bits = chips.bit_length() - 1

    def flipped(index, bits):
        return sum((index >> t & 1) << (bits - 1 - t) for t in range(bits))

    def piece_of(ch, core, j, z):
        part, at = divmod(z, n_sub // 2)
        return gathered_s[ch, core, part, flipped(j, chip_bits) if part else j, at].astype(F32)

    for ch, matrix in enumerate((3, 0)):
        for j in range(chips):
            for z in range(n_sub):
                columns = slice(z * part_lanes, (z + 1) * part_lanes)
                span = slice(2 * j * part_rows, 2 * (j + 1) * part_rows)
                both = jnp.concatenate([piece_of(ch, core, j, z) for core in range(2)], axis=0)
                if ch == 0:
                    w_s[matrix, span, columns] = both
                else:
                    w_s[matrix, columns, span] = both.T
        store(w_s.at[matrix], weight_grads.at[matrix])
    for m in range(4):
        rows_of = part_rows // 2
        for core in range(2):
            for j in range(chips):
                at = m % 2 * half_rows + core * half_rows // 2 + j * rows_of
                for z in range(n_sub):
                    columns = slice(z * part_lanes, (z + 1) * part_lanes)
                    w_s[1 + m // 2, at:at + rows_of, columns] = mgathered_s[m, core, j, z].astype(F32)
        at = pl.ds(m % 2 * half_rows, half_rows)
        store(w_s.at[1 + m // 2, at], weight_grads.at[1 + m // 2, at])
    for move in stores:
        move.wait()


def shards(
    n_grid, n_sub,
    grid_x, mesh_h, gain_grid, gain_mesh, w_query, w_key, w_value, w_out,
    edge_bias, neighbours, valid, send_rows, out_grad,
):
    points, width = grid_x.shape
    nodes = mesh_h.shape[0]
    slots_per = send_rows.shape[3]
    fanout = neighbours.shape[1]
    slots = 3 * n_sub * slots_per
    chips = n_grid // 2
    chunks = 2
    half_rows = width // 2
    block, lanes = half_rows // chips, width // n_sub
    anywhere = pl.BlockSpec(memory_space=pl.ANY)
    inside = pl.BlockSpec(memory_space=pltpu.VMEM)
    dma = pltpu.SemaphoreType.DMA
    gain_grid, gain_mesh = gain_grid.reshape(1, width), gain_mesh.reshape(1, width)
    operands = (
        grid_x, mesh_h, gain_grid, gain_mesh, w_query, w_key, w_value, w_out,
        edge_bias, neighbours, valid, send_rows, out_grad,
    )
    blocks = (3, n_sub, slots_per, width)
    node_rows = pltpu.VMEM((nodes, width), BF16)
    slot_rows = pltpu.VMEM((slots, width), BF16)
    chip_bits = chips.bit_length() - 1
    pieces = (chunks, 2, 2, chips, n_sub // 2, block, lanes)
    mpieces = (4, 2, chips, n_sub, block // 2, lanes)
    kept = 2 * (points * width + 2 * nodes * width + 4 * width * width) + 2**16
    found = pl.pallas_call(
        functools.partial(layer, n_grid, n_sub),
        in_specs=[anywhere] * len(operands),
        out_specs=[inside] * 5,
        out_shape=[
            pltpu.VMEM((points, width), BF16),
            pltpu.VMEM(pieces, BF16),
            pltpu.VMEM(mpieces, BF16),
            node_rows, node_rows,
        ],
        scratch_shapes=[pltpu.VMEM(a.shape, a.dtype) for a in operands] + [
            pltpu.VMEM(blocks, BF16), pltpu.VMEM(blocks, BF16), pltpu.VMEM((width, slots), BF16),
            pltpu.VMEM(blocks, BF16), pltpu.VMEM(blocks, BF16), pltpu.VMEM((1, slots), jnp.int32),
            pltpu.VMEM((2, points // 2, 2 * n_sub * slots_per), BF16), pltpu.VMEM((points, 1), F32),
            pltpu.VMEM((nodes * ROWS, LANES), F32),
            pltpu.VMEM((slots // LANES, nodes * 8, LANES), F32),
            pltpu.VMEM((nodes, fanout), jnp.int32),
            node_rows, node_rows, slot_rows, slot_rows, node_rows, node_rows,
            slot_rows, slot_rows,
            pltpu.VMEM((2, chips, nodes, width), BF16),
            pltpu.VMEM((2, chips, nodes, width // chips), BF16),
            pltpu.VMEM((2, chips, nodes, width // chips), BF16),
            pltpu.VMEM((2, 2, block, width), F32),
            pltpu.VMEM((2, block, width), BF16), pltpu.VMEM((2, block, width), BF16),
            pltpu.VMEM((4, 2, half_rows // 2, width), F32),
            pltpu.VMEM((4, half_rows // 2, width), BF16), pltpu.VMEM((4, half_rows // 2, width), BF16),
            pltpu.VMEM((4, chips, block // 2, width), F32),
            pltpu.VMEM((4, chips, block // 2, width), BF16),
            pltpu.VMEM((4, chips, block // 2, width), BF16),
            pltpu.VMEM((4, n_sub, block // 2, lanes), F32),
            pltpu.VMEM((4, n_sub, block // 2, lanes), BF16),
            pltpu.VMEM((4, n_sub, block // 2, lanes), BF16),
            pltpu.VMEM(mpieces[:1] + mpieces[2:], BF16),
            pltpu.VMEM((chunks, n_sub, block, lanes), F32),
            pltpu.VMEM((chunks, n_sub, block, lanes), BF16),
            pltpu.VMEM((chunks, n_sub, block, lanes), BF16),
            pltpu.VMEM(pieces[:1] + pieces[2:], BF16),
            dma((len(operands),)),
            dma((3 * n_sub,)), dma((3 * n_sub,)), dma((3 * n_sub,)), dma((3 * n_sub,)),
            dma((2, chips)), dma((2, chips)), dma((2, chips)), dma((2, chips)),
            dma((chunks,)), dma((chunks,)),
            dma((4,)), dma((4,)), dma((4, chips)), dma((4, chips)), dma((4, n_sub)), dma((4, n_sub)),
            dma((4, n_sub)), dma((4, n_sub)), dma((4, chips)), dma((4, chips)), dma((4,)), dma((4,)),
            dma((chunks, n_sub)), dma((chunks, n_sub)),
            dma((chunks, n_sub)), dma((chunks, n_sub)),
            dma((chunks, 2, chips)), dma((chunks, 2, chips)),
            dma((chunks,)), dma((chunks,)),
        ],
        compiler_params=pltpu.CompilerParams(
            collective_id=0, has_side_effects=True, vmem_limit_bytes=VMEM_BYTES - kept
        ),
        name="layer",
    )(*operands)
    gx, gathered, mgathered, mo, mg = found
    return pl.pallas_call(
        finish,
        in_specs=[inside] * 5,
        out_specs=[anywhere] * 4,
        out_shape=[
            jax.ShapeDtypeStruct((nodes, width), BF16),
            jax.ShapeDtypeStruct((nodes, width), BF16),
            jax.ShapeDtypeStruct((points, width), BF16),
            jax.ShapeDtypeStruct((4, width, width), F32),
        ],
        scratch_shapes=[pltpu.VMEM((4, width, width), F32), dma((9,))],
        compiler_params=pltpu.CompilerParams(vmem_limit_bytes=LIMIT),
        name="finish",
    )(gathered, mgathered, mo, mg, gx)


def solution(mesh):
    by_device = P(("grid", "sub"), None)
    in_specs = (
        by_device, by_device, P(), P(), P(), P(), P(), P(), by_device, by_device, by_device,
        P(("grid", "sub"), None, None, None), by_device,
    )
    out_specs = (by_device, by_device, by_device, P())
    body = functools.partial(shards, mesh.shape["grid"], mesh.shape["sub"])
    return jax.shard_map(body, mesh=mesh, in_specs=in_specs, out_specs=out_specs, check_vma=False)
```
